8 devices in a mesh: nodes: 8 (over z, y, x, core).
Axes of the slice: x: 2, y: 2, z: 1, core: 2. Of those that a mesh axis runs over, the one named last changes fastest.
Arguments:
- adjacency: bfloat16 [16384, 16384], P('nodes')
- features: bfloat16 [16384, 602], P('nodes')
- w_hidden: float32 [602, 128], replicated
- w_output: float32 [128, 41], replicated
- labels: int32 [16384], P('nodes')
- train_mask: int32 [16384], P('nodes')
- block_mask: int32 [8, 8], replicated
Outputs:
- output 1: float32 [], replicated
- output 2: float32 [602, 128], replicated
- output 3: float32 [128, 41], replicated
All inputs are finite; a program needn't handle non-finite values.
Results may differ from the reference program's by a relative error of at most 0.001.
Values are sent between devices in bfloat16 or wider.
A program may use at most 1 GiB of HBM per device.

```python
import jax
import jax.numpy as jnp
from jax import lax

NUM_NODES = 16384
BLOCKS = 8
F_IN = 602
HID = 128
CLASSES = 41
EDGE_PERCENT = 15
BLOCK_ROWS = NUM_NODES // BLOCKS


def setup_inputs(seed: int = 0) -> dict:
    keys = jax.random.split(jax.random.key(seed), 9)
    thresholds = jax.random.randint(keys[0], (BLOCKS, 1), BLOCKS // 8, BLOCKS + 1, dtype=jnp.int32)
    block_draw = jax.random.randint(keys[1], (BLOCKS, BLOCKS), 0, BLOCKS, dtype=jnp.int32)
    block_mask = jnp.maximum((block_draw < thresholds).astype(jnp.int32), jnp.eye(BLOCKS, dtype=jnp.int32))
    col_ids = jnp.arange(NUM_NODES, dtype=jnp.int32)

    def edge_rows(block_id):
        edge_draw = jax.random.randint(jax.random.fold_in(keys[2], block_id), (BLOCK_ROWS, NUM_NODES), 0, 100, dtype=jnp.int32)
        row_ids = block_id * BLOCK_ROWS + jnp.arange(BLOCK_ROWS, dtype=jnp.int32)
        col_keep = jnp.repeat(block_mask[block_id], BLOCK_ROWS) > 0
        edge_on = ((edge_draw < EDGE_PERCENT) | (row_ids[:, None] == col_ids[None, :])) & col_keep[None, :]
        raw_weight = edge_on.astype(jnp.float32)
        return (raw_weight / jnp.sum(raw_weight, axis=1, keepdims=True)).astype(jnp.bfloat16)

    adjacency = lax.map(edge_rows, jnp.arange(BLOCKS, dtype=jnp.int32)).reshape(NUM_NODES, NUM_NODES)
    centers = jax.random.normal(keys[3], (BLOCKS, F_IN), jnp.float32)
    noise = jax.random.normal(keys[4], (NUM_NODES, F_IN), jnp.float32)
    features = (jnp.repeat(centers, BLOCK_ROWS, axis=0) + noise).astype(jnp.bfloat16)
    w_hidden = jax.random.normal(keys[5], (F_IN, HID), jnp.float32) * (F_IN ** -0.5 * BLOCKS ** 0.25)
    w_output = jax.random.normal(keys[6], (HID, CLASSES), jnp.float32) * (2.0 * HID ** -0.5)
    labels = jax.random.randint(keys[7], (NUM_NODES,), 0, CLASSES, dtype=jnp.int32)
    label_draw = jax.random.randint(keys[8], (NUM_NODES,), 0, 100, dtype=jnp.int32)
    train_mask = jnp.maximum((label_draw < 40).astype(jnp.int32), (col_ids == 0).astype(jnp.int32))
    return dict(adjacency=adjacency, features=features, w_hidden=w_hidden, w_output=w_output, labels=labels, train_mask=train_mask, block_mask=block_mask)


def masked_product(adj_blocks, block_mask, values):
    width = values.shape[-1]
    value_blocks = values.reshape(BLOCKS, BLOCK_ROWS, width)

    def one_block(block_item):
        adj_rows, mask_row = block_item
        scaled = value_blocks * mask_row.astype(values.dtype)[:, None, None]
        return jnp.dot(adj_rows, scaled.reshape(NUM_NODES, width), preferred_element_type=jnp.float32)

    return lax.map(one_block, (adj_blocks, block_mask)).reshape(NUM_NODES, width)


def masked_transpose_product(adj_blocks, block_mask, grads):
    width = grads.shape[-1]
    grad_blocks = grads.reshape(BLOCKS, BLOCK_ROWS, width)

    def add_block(running_sum, block_item):
        adj_rows, mask_row, grad_rows = block_item
        contrib = jnp.dot(adj_rows.T, grad_rows, preferred_element_type=jnp.float32)
        contrib = contrib.reshape(BLOCKS, BLOCK_ROWS, width) * mask_row.astype(jnp.float32)[:, None, None]
        return running_sum + contrib.reshape(NUM_NODES, width), None

    start_sum = jnp.zeros((NUM_NODES, width), jnp.float32)
    total_sum, _ = lax.scan(add_block, start_sum, (adj_blocks, block_mask, grad_blocks))
    return total_sum


def reference(adjacency, features, w_hidden, w_output, labels, train_mask, block_mask):
    adj_blocks = adjacency.reshape(BLOCKS, BLOCK_ROWS, NUM_NODES)
    w_hidden_bf = w_hidden.astype(jnp.bfloat16)
    w_output_bf = w_output.astype(jnp.bfloat16)
    proj_one = jnp.dot(features, w_hidden_bf, preferred_element_type=jnp.float32).astype(jnp.bfloat16)
    agg_one = masked_product(adj_blocks, block_mask, proj_one)
    hidden = jnp.maximum(agg_one, 0.0).astype(jnp.bfloat16)
    proj_two = jnp.dot(hidden, w_output_bf, preferred_element_type=jnp.float32).astype(jnp.bfloat16)
    logits = masked_product(adj_blocks, block_mask, proj_two)
    label_weight = train_mask.astype(jnp.float32)
    label_count = jnp.sum(label_weight)
    log_norm = jax.nn.logsumexp(logits, axis=-1)
    one_hot = (labels[:, None] == jnp.arange(CLASSES)[None, :]).astype(jnp.float32)
    picked = jnp.sum(logits * one_hot, axis=-1)
    mean_loss = jnp.sum(label_weight * (log_norm - picked)) / label_count
    probabilities = jnp.exp(logits - log_norm[:, None])
    grad_logits = ((probabilities - one_hot) * (label_weight / label_count)[:, None]).astype(jnp.bfloat16)
    grad_proj_two = masked_transpose_product(adj_blocks, block_mask, grad_logits).astype(jnp.bfloat16)
    grad_w_output = jnp.dot(hidden.T, grad_proj_two, preferred_element_type=jnp.float32)
    grad_hidden = jnp.dot(grad_proj_two, w_output_bf.T, preferred_element_type=jnp.float32)
    grad_agg = jnp.where(agg_one > 0, grad_hidden, 0.0).astype(jnp.bfloat16)
    grad_proj_one = masked_transpose_product(adj_blocks, block_mask, grad_agg).astype(jnp.bfloat16)
    grad_w_hidden = jnp.dot(features.T, grad_proj_one, preferred_element_type=jnp.float32)
    return (mean_loss, grad_w_hidden, grad_w_output)
```

```python
import jax
import jax.numpy as jnp
from jax import lax
from jax.experimental import pallas as pl
from jax.experimental.pallas import tpu as pltpu
from jax.sharding import PartitionSpec as P

AXIS_NAME = 'nodes'
MESH = pl.DeviceIdType.MESH
F32, BF16 = jnp.float32, jnp.bfloat16
DEVICES = 8
ROWS = 2048
NODES = DEVICES * ROWS
F_IN = 602
F_PAD = 640
HID = 128
CLASSES = 41
C_PAD = 48
HALF = ROWS // 2
SLOTS = 6
CHUNKS = NODES // HALF
SLICE = HID // DEVICES
NT = (((1,), (1,)), ((), ()))


def step_kernel(adj, feat, wh, wo, labels, mask, block_mask, loss_out, gwh_out, gwo_out,
                abuf, xbuf, acc, yall, y2all, ymask, hid, z1t, z2t, wot, lhs1, lhs2, cnt,
                pa, ra, fa, ia, pb, rb, fb, ib, lossall, gwoall, gpart, garr, gred, gfull,
                asem, xsem, ssem, rsem):
    me = lax.axis_index(AXIS_NAME)
    bits = (lax.rem(me, 2), lax.rem(me // 2, 2), me // 4)

    def partner(k):
        return lax.rem(bits[0] + k, 2) + 2 * lax.rem(bits[1] + k // 2, 2) + 4 * lax.rem(bits[2] + k // 4, 2)

    peers = [partner(k) for k in range(DEVICES)]

    def block_half(g):
        back = g // (2 * CHUNKS)
        c = lax.rem(g, CHUNKS)
        k = back * (DEVICES - 1 - c // 2) + (1 - back) * (c // 2)
        return k, lax.rem(c, 2)

    def fetch(g):
        k, h = block_half(g)
        col = pl.multiple_of(partner(k) * ROWS + h * HALF, HALF)
        slot = lax.rem(g, SLOTS)
        return pltpu.make_async_copy(adj.at[:, pl.ds(col, HALF)], abuf.at[slot], asem.at[slot])

    def remote(i, src, dst, k):
        return pltpu.make_async_remote_copy(src_ref=src, dst_ref=dst, send_sem=ssem.at[i], recv_sem=rsem.at[i],
                                            device_id=(peers[k],), device_id_type=MESH)

    for g in range(SLOTS):
        fetch(jnp.int32(g)).start()
    xcopy = pltpu.make_async_copy(feat, xbuf, xsem.at[0])
    xcopy.start()
    barrier = pltpu.get_barrier_semaphore()
    for k in range(1, DEVICES):
        pl.semaphore_signal(barrier, inc=1, device_id=(peers[k],), device_id_type=MESH)

    wot[...] = jnp.zeros_like(wot)
    wot[:, :CLASSES] = wo[...]
    wo_pad = wot[...]
    wot_bf = wo_pad.T[:C_PAD].astype(BF16)
    wo_bf = wo_pad[:, :C_PAD].astype(BF16)
    weight = mask[...].astype(F32)
    cnt[0] = jnp.broadcast_to(jnp.sum(weight, axis=1, keepdims=True), (8, 128))
    xcopy.wait()
    wh_bf = wh[...].astype(BF16)
    yall[0] = jnp.dot(xbuf[...], wh_bf, preferred_element_type=F32).astype(BF16)
    pl.semaphore_wait(barrier, DEVICES - 1)

    def gather_copies(base, y, half):
        h0, h1 = 0, 1
        return [
            remote(base + 0, y.at[0], y.at[1], 1),
            remote(base + 1, half(y, 0, h0), half(y, 2, h0), 2),
            remote(base + 2, half(y, 0, h1), half(y, 2, h1), 2),
            remote(base + 3, half(y, 0, h1), half(y, 4, h1), 4),
            remote(base + 4, half(y, 0, h0), half(y, 4, h0), 4),
            remote(base + 5, half(y, 2, h0), half(y, 3, h0), 1),
            remote(base + 6, half(y, 2, h1), half(y, 3, h1), 1),
            remote(base + 7, half(y, 4, h0), half(y, 5, h0), 1),
            remote(base + 8, half(y, 4, h1), half(y, 5, h1), 1),
            remote(base + 9, half(y, 2, h0), half(y, 6, h0), 4),
            remote(base + 10, half(y, 4, h1), half(y, 6, h1), 2),
            remote(base + 11, half(y, 6, h0), half(y, 7, h0), 1),
            remote(base + 12, half(y, 6, h1), half(y, 7, h1), 1),
        ]

    def row_half(y, slot, h):
        return y.at[slot, pl.ds(h * HALF, HALF), :]

    def col_half(y, slot, h):
        return y.at[slot, :, pl.ds(h * HALF, HALF)]

    def gather_events(copies, c):
        def events(at, waits, starts):
            @pl.when(c == at)
            def _():
                for w in waits:
                    copies[w].wait_recv()
                for s in starts:
                    copies[s].start()
        events(2, (0,), ())
        events(4, (1,), (9, 5))
        events(4, (3,), (10, 8))
        events(5, (2, 4), (6, 7))
        events(6, (5, 6), ())
        events(10, (8, 7), ())
        events(12, (9,), (11,))
        events(12, (10,), (12,))
        events(14, (11, 12), ())

    def mask_value(k):
        return block_mask[me, partner(k)].astype(F32)

    def next_fetch(g):
        @pl.when(g + SLOTS < 4 * CHUNKS)
        def _():
            fetch(g + SLOTS).start()

    copies = gather_copies(0, yall, row_half)
    for i in range(5):
        copies[i].start()
    count_copies = [remote(13 + k, cnt.at[0], cnt.at[k], k) for k in range(1, DEVICES)]
    for copy in count_copies:
        copy.start()
    acc[...] = jnp.zeros_like(acc)

    def pass1(c, carry):
        gather_events(copies, c)
        k, h = block_half(c)
        rows = pl.ds(pl.multiple_of(h * HALF, HALF), HALF)
        ymask[...] = (yall[k, rows, :].astype(F32) * mask_value(k)).astype(BF16)
        fetch(c).wait()
        acc[...] += jnp.dot(abuf[lax.rem(c, SLOTS)], ymask[...], preferred_element_type=F32)
        next_fetch(c)
        return carry
    lax.fori_loop(0, CHUNKS, pass1, 0)

    hid[...] = jnp.maximum(acc[...], 0.0).astype(BF16)
    y2all[0] = lax.dot_general(wot_bf, hid[...], NT, preferred_element_type=F32).astype(BF16)
    for copy in copies + count_copies:
        copy.wait_send()

    copies2 = gather_copies(21, y2all, col_half)
    for i in range(5):
        copies2[i].start()

    def turn(i, carry):
        at = pl.ds(pl.multiple_of(i * 128, 128), 128)
        z1t[:, at] = acc[at, :].T
        return carry
    lax.fori_loop(0, ROWS // 128, turn, 0)
    acc[...] = jnp.zeros_like(acc)

    def pass2(c, carry):
        gather_events(copies2, c)
        k, h = block_half(c)
        cols = pl.ds(pl.multiple_of(h * HALF, HALF), HALF)
        y2mask = (y2all[k, :, cols].astype(F32) * mask_value(k)).astype(BF16)
        g = c + CHUNKS
        fetch(g).wait()
        acc[:, :C_PAD] += lax.dot_general(abuf[lax.rem(g, SLOTS)], y2mask, NT, preferred_element_type=F32)
        next_fetch(g)
        return carry
    lax.fori_loop(0, CHUNKS, pass2, 0)
    for copy in copies2:
        copy.wait_send()

    def turn2(i, carry):
        at = pl.ds(pl.multiple_of(i * 128, 128), 128)
        z2t[:, at] = acc[at, :].T[:C_PAD]
        return carry
    lax.fori_loop(0, ROWS // 128, turn2, 0)
    for copy in count_copies:
        copy.wait_recv()
    label_count = cnt[0, 0:1, 0:1]
    for k in range(1, DEVICES):
        label_count = label_count + cnt[k, 0:1, 0:1]
    loss = jnp.zeros((1, 1), F32)
    for q in range(4):
        at = pl.ds(q * 512, 512)
        z = z2t[:, at]
        row = lax.broadcasted_iota(jnp.int32, (C_PAD, 512), 0)
        z = jnp.where(row < CLASSES, z, -jnp.inf)
        top = jnp.max(z, axis=0, keepdims=True)
        log_norm = jnp.log(jnp.sum(jnp.exp(z - top), axis=0, keepdims=True)) + top
        hot = row == labels[:, at]
        picked = jnp.sum(jnp.where(hot, z, 0.0), axis=0, keepdims=True)
        w = mask[:, at].astype(F32)
        loss = loss + jnp.sum(w * (log_norm - picked), axis=1, keepdims=True)
        prob = jnp.exp(z - log_norm)
        lhs1[:, at] = ((prob - hot.astype(F32)) * (w / label_count)).astype(BF16)
    lossall[me] = jnp.broadcast_to(loss, (8, 128))

    def scatter_copies(base, p, r, f, ix):
        h0, h1 = pl.ds(0, HALF), pl.ds(HALF, HALF)
        return [
            remote(base + 0, p.at[7], r.at[3], 1),
            remote(base + 1, p.at[6, :, h0], f.at[0], 2),
            remote(base + 2, p.at[6, :, h1], f.at[1], 4),
            remote(base + 3, p.at[5], r.at[2], 1),
            remote(base + 4, p.at[4, :, h1], ix.at[1, 1], 4),
            remote(base + 5, p.at[3], r.at[1], 1),
            remote(base + 6, p.at[2, :, h0], ix.at[0, 0], 2),
            remote(base + 7, p.at[1], r.at[0], 1),
            remote(base + 8, p.at[4, :, h0], ix.at[1, 0], 4),
            remote(base + 9, p.at[2, :, h1], ix.at[0, 1], 2),
        ]

    def scatter_events(copies, p, r, f, c, pass_on_at):
        h0, h1 = pl.ds(0, HALF), pl.ds(HALF, HALF)

        def join(k, wait):
            copies[wait].wait_recv()
            p[k] = p[k] + r[k // 2]

        @pl.when(c == 1)
        def _():
            copies[0].start()

        @pl.when(c == 3)
        def _():
            join(6, 0)
            copies[1].start()
            copies[2].start()

        @pl.when(c == 5)
        def _():
            copies[3].start()

        @pl.when(c == 7)
        def _():
            join(4, 3)
            copies[4].start()

        @pl.when(c == 9)
        def _():
            copies[5].start()

        @pl.when(c == 11)
        def _():
            join(2, 5)
            copies[6].start()

        @pl.when(c == 13)
        def _():
            copies[7].start()

        @pl.when(c == pass_on_at)
        def _():
            copies[1].wait_recv()
            p[4, :, h0] = p[4, :, h0] + f[0]
            copies[8].start()
            copies[2].wait_recv()
            p[2, :, h1] = p[2, :, h1] + f[1]
            copies[9].start()

        @pl.when(c == CHUNKS - 1)
        def _():
            join(0, 7)

    def scatter_result(copies, p, ix, h):
        at = pl.ds(h * HALF, HALF)
        return (p[0, :, at] + ix[0, h] + ix[1, h]).astype(BF16)

    copies3 = scatter_copies(34, pa, ra, fa, ia)

    def pass3(c, carry):
        g = c + 2 * CHUNKS
        k, h = block_half(g)
        cols = pl.ds(pl.multiple_of(h * HALF, HALF), HALF)
        fetch(g).wait()
        part = jnp.dot(lhs1[...], abuf[lax.rem(g, SLOTS)], preferred_element_type=F32)
        pa[k, :, cols] = part * mask_value(k)
        next_fetch(g)
        scatter_events(copies3, pa, ra, fa, c, 11)
        return carry
    lax.fori_loop(0, CHUNKS, pass3, 0)
    for i in (6, 9, 4, 8):
        copies3[i].wait_recv()
    for copy in copies3:
        copy.wait_send()
    d2t = jnp.concatenate([scatter_result(copies3, pa, ia, h) for h in range(2)], axis=1)
    gwoall[me] = jnp.dot(d2t, hid[...], preferred_element_type=F32)
    back = jnp.dot(wo_bf, d2t, preferred_element_type=F32)
    lhs2[...] = jnp.where(z1t[...] > 0.0, back, 0.0).astype(BF16)

    small_copies = []
    for k in range(1, DEVICES):
        small_copies.append((remote(44 + k, lossall.at[me], lossall.at[me], k), remote(52 + k, gwoall.at[me], gwoall.at[me], k)))
    for pair in small_copies:
        for copy in pair:
            copy.start()

    copies4 = scatter_copies(60, pb, rb, fb, ib)

    def pass4(c, carry):
        g = c + 3 * CHUNKS
        k, h = block_half(g)
        cols = pl.ds(pl.multiple_of(h * HALF, HALF), HALF)
        fetch(g).wait()
        part = jnp.dot(lhs2[...], abuf[lax.rem(g, SLOTS)], preferred_element_type=F32)
        pb[k, :, cols] = part * mask_value(k)
        next_fetch(g)
        scatter_events(copies4, pb, rb, fb, c, CHUNKS - 1)
        return carry
    lax.fori_loop(0, CHUNKS, pass4, 0)

    for pair in small_copies:
        for copy in pair:
            copy.wait()
    loss = lossall[0, 0:1, 0:1]
    gwo = gwoall[0]
    for d in range(1, DEVICES):
        loss = loss + lossall[d, 0:1, 0:1]
        gwo = gwo + gwoall[d]
    loss_out[...] = loss / label_count
    wot[...] = jnp.zeros_like(wot)
    wot[:C_PAD, :] = gwo
    gwo_out[...] = wot[...].T[:, :CLASSES]

    for i in (6, 9, 4, 8):
        copies4[i].wait_recv()
    for copy in copies4:
        copy.wait_send()
    d1t = jnp.concatenate([scatter_result(copies4, pb, ib, h) for h in range(2)], axis=1)
    gpart[:, :F_IN] = jnp.dot(d1t, xbuf[...], preferred_element_type=F32)

    mine = pl.ds(pl.multiple_of(me * SLICE, SLICE), SLICE)
    parts = []
    for k in range(1, DEVICES):
        theirs = pl.ds(pl.multiple_of(peers[k] * SLICE, SLICE), SLICE)
        parts.append(remote(70 + k, gpart.at[theirs, :], garr.at[me], k))
    for copy in parts:
        copy.start()
    garr[me] = gpart[mine, :]
    for copy in parts:
        copy.wait()
    total = garr[0]
    for d in range(1, DEVICES):
        total = total + garr[d]
    gred[...] = total
    wholes = [remote(78 + k, gred, gfull.at[mine, :], k) for k in range(1, DEVICES)]
    for copy in wholes:
        copy.start()
    gfull[mine, :] = total
    for copy in wholes:
        copy.wait()
    for i in range(F_PAD // 128):
        at = pl.ds(i * 128, 128)
        n = min(128, F_IN - i * 128)
        gwh_out[i * 128:i * 128 + n, :] = gfull[:, at].T[:n]


def device_step(adj, feat, w_hidden, w_output, labels, train_mask, block_mask):
    vmem = pl.BlockSpec(memory_space=pltpu.VMEM)
    hbm = pl.BlockSpec(memory_space=pl.ANY)
    v = pltpu.VMEM
    copies = 86
    loss, gwh, gwo = pl.pallas_call(
        step_kernel,
        out_shape=(jax.ShapeDtypeStruct((1, 1), F32), jax.ShapeDtypeStruct((F_IN, HID), F32), jax.ShapeDtypeStruct((HID, CLASSES), F32)),
        in_specs=[hbm, hbm, vmem, vmem, vmem, vmem, pl.BlockSpec(memory_space=pltpu.SMEM)],
        out_specs=(vmem, vmem, vmem),
        scratch_shapes=[
            v((SLOTS, ROWS, HALF), BF16), v((ROWS, F_IN), BF16), v((ROWS, HID), F32),
            v((DEVICES, ROWS, HID), BF16), v((DEVICES, C_PAD, ROWS), BF16), v((HALF, HID), BF16), v((ROWS, HID), BF16),
            v((HID, ROWS), F32), v((C_PAD, ROWS), F32), v((128, 128), F32), v((C_PAD, ROWS), BF16), v((HID, ROWS), BF16),
            v((DEVICES, 8, 128), F32),
            v((DEVICES, C_PAD, ROWS), F32), v((4, C_PAD, ROWS), F32), v((2, C_PAD, HALF), F32), v((2, 2, C_PAD, HALF), F32),
            v((DEVICES, HID, ROWS), F32), v((4, HID, ROWS), F32), v((2, HID, HALF), F32), v((2, 2, HID, HALF), F32),
            v((DEVICES, 8, 128), F32), v((DEVICES, C_PAD, HID), F32),
            v((HID, F_PAD), F32), v((DEVICES, SLICE, F_PAD), F32), v((SLICE, F_PAD), F32), v((HID, F_PAD), F32),
            pltpu.SemaphoreType.DMA((SLOTS,)), pltpu.SemaphoreType.DMA((1,)),
            pltpu.SemaphoreType.DMA((copies,)), pltpu.SemaphoreType.DMA((copies,)),
        ],
        compiler_params=pltpu.CompilerParams(collective_id=0, has_side_effects=True, vmem_limit_bytes=67043328),
        name='gcn_step',
    )(adj, feat, w_hidden, w_output, labels.reshape(1, ROWS), train_mask.reshape(1, ROWS), block_mask)
    return loss[0, 0], gwh, gwo


def solution(mesh):
    row_spec = P(AXIS_NAME, None)
    vec_spec = P(AXIS_NAME)
    return jax.shard_map(device_step, mesh=mesh, in_specs=(row_spec, row_spec, P(), P(), vec_spec, vec_spec, P()), out_specs=(P(), P(), P()), check_vma=False)
```

```python
import jax
import jax.numpy as jnp
from jax import lax
from jax.experimental import pallas as pl
from jax.experimental.pallas import tpu as pltpu
from jax.sharding import PartitionSpec as P

AXIS_NAME = 'nodes'
MESH = pl.DeviceIdType.MESH
F32, BF16 = jnp.float32, jnp.bfloat16
DEVICES = 8
ROWS = 2048
NODES = DEVICES * ROWS
F_IN = 602
HID = 128
CLASSES = 41
C_PAD = 48
HALF = ROWS // 2
QUART = ROWS // 4
SLOTS = 6
CHUNKS = NODES // HALF
SUM_ROWS = 672
GWO_ROW = 608
LOSS_ROW = GWO_ROW + C_PAD
NT = (((1,), (1,)), ((), ()))


def step_kernel(adj, feat, wh, wo, labels, mask, block_mask, loss_out, gwh_out, gwo_out,
                abuf, xbuf, acc, yall, y2all, ymask, hid, z1t, z2t, wpad, lhs1, lhs2, cnt,
                pa, ra, fa, ia, pb, rb, fb, ib, gpart, gpair, gacross, gback,
                asem, xsem, ssem, rsem):
    me = lax.axis_index(AXIS_NAME)
    bits = (lax.rem(me, 2), lax.rem(me // 2, 2), me // 4)

    def partner(k):
        return lax.rem(bits[0] + k, 2) + 2 * lax.rem(bits[1] + k // 2, 2) + 4 * lax.rem(bits[2] + k // 4, 2)

    peers = [partner(k) for k in range(DEVICES)]

    def block_half(g):
        back = g // (2 * CHUNKS)
        c = lax.rem(g, CHUNKS)
        q, r = c // 4, lax.rem(c, 4)
        forth_k = 2 * q + r // 2
        forth_h = lax.rem(r, 2)
        back_k = DEVICES - 1 - 2 * q - lax.rem(r, 2)
        back_h = r // 2
        return back * back_k + (1 - back) * forth_k, back * back_h + (1 - back) * forth_h

    def fetch(g):
        k, h = block_half(g)
        col = pl.multiple_of(partner(k) * ROWS + h * HALF, HALF)
        slot = lax.rem(g, SLOTS)
        return pltpu.make_async_copy(adj.at[:, pl.ds(col, HALF)], abuf.at[slot], asem.at[slot])

    used = [0]

    def remote(src, dst, k):
        i = used[0]
        used[0] += 1
        return pltpu.make_async_remote_copy(src_ref=src, dst_ref=dst, send_sem=ssem.at[i], recv_sem=rsem.at[i],
                                            device_id=(peers[k],), device_id_type=MESH)

    xcopy = pltpu.make_async_copy(feat, xbuf, xsem.at[0])
    xcopy.start()
    for g in range(SLOTS):
        fetch(jnp.int32(g)).start()
    barrier = pltpu.get_barrier_semaphore()
    for k in range(1, DEVICES):
        pl.semaphore_signal(barrier, inc=1, device_id=(peers[k],), device_id_type=MESH)

    wpad[...] = jnp.zeros_like(wpad)
    wpad[:CLASSES, :] = wo[...]
    wot_bf = wpad[:C_PAD, :].astype(BF16)
    wo_bf = wpad[...].T[:, :C_PAD].astype(BF16)
    wh_t = wh[...].T.astype(BF16)
    weight = mask[...].astype(F32)
    cnt[0] = jnp.broadcast_to(jnp.sum(weight, axis=1, keepdims=True), (8, 128))
    xcopy.wait()
    yall[0] = jnp.dot(wh_t, xbuf[...], preferred_element_type=F32).astype(BF16)
    pl.semaphore_wait(barrier, DEVICES - 1)

    def gather_copies(y):
        def half(k, h):
            return y.at[k, :, pl.ds(h * HALF, HALF)]

        def quart(k, q):
            return y.at[k, :, pl.ds(q * QUART, QUART)]

        copies = {'own': remote(y.at[0], y.at[1], 1)}
        for h in range(2):
            copies['x', h] = remote(half(0, h), half(2, h), 2)
            copies['y', h] = remote(half(0, h), half(4, h), 4)
            copies['x core', h] = remote(half(2, h), half(3, h), 1)
            copies['y core', h] = remote(half(4, h), half(5, h), 1)
            copies['xy', h] = remote(quart(2, 2 * h), quart(6, 2 * h), 4)
            copies['yx', h] = remote(quart(4, 2 * h + 1), quart(6, 2 * h + 1), 2)
            copies['xy core', h] = remote(half(6, h), half(7, h), 1)
        return copies

    def gather_start(copies):
        for name in (('x', 0), ('y', 0), ('x', 1), ('y', 1), 'own'):
            copies[name].start()

    def gather_events(copies, c):
        @pl.when(c == 2)
        def _():
            copies['own'].wait_recv()

        for h in range(2):
            @pl.when(c == 4 + h)
            def _(h=h):
                copies['x', h].wait_recv()
                copies['xy', h].start()
                copies['x core', h].start()
                copies['y', h].wait_recv()
                copies['yx', h].start()
                copies['y core', h].start()

            @pl.when(c == 6 + h)
            def _(h=h):
                copies['x core', h].wait_recv()

            @pl.when(c == 10 + h)
            def _(h=h):
                copies['y core', h].wait_recv()

            @pl.when(c == 12 + h)
            def _(h=h):
                copies['xy', h].wait_recv()
                copies['yx', h].wait_recv()
                copies['xy core', h].start()

            @pl.when(c == 14 + h)
            def _(h=h):
                copies['xy core', h].wait_recv()

    def mask_value(k):
        return block_mask[me, partner(k)].astype(F32)

    def next_fetch(g):
        @pl.when(g + SLOTS < 4 * CHUNKS)
        def _():
            fetch(g + SLOTS).start()

    def masked(y, k, h):
        cols = pl.ds(pl.multiple_of(h * HALF, HALF), HALF)
        return (y[k, :, cols].astype(F32) * mask_value(k)).astype(BF16)

    copies1 = gather_copies(yall)
    gather_start(copies1)
    acc[...] = jnp.zeros_like(acc)

    def pass1(c, carry):
        gather_events(copies1, c)
        k, h = block_half(c)
        ymask[...] = masked(yall, k, h)
        fetch(c).wait()
        acc[...] += lax.dot_general(abuf[lax.rem(c, SLOTS)], ymask[...], NT, preferred_element_type=F32)
        next_fetch(c)
        return carry
    lax.fori_loop(0, CHUNKS, pass1, 0)

    hid[...] = jnp.maximum(acc[...], 0.0).astype(BF16)
    y2all[0] = lax.dot_general(wot_bf, hid[...], NT, preferred_element_type=F32).astype(BF16)

    copies2 = gather_copies(y2all)
    gather_start(copies2)
    count_copies = [remote(cnt.at[0], cnt.at[k], k) for k in range(1, DEVICES)]
    for copy in count_copies:
        copy.start()
    for copy in copies1.values():
        copy.wait_send()

    def turn(i, carry):
        at = pl.ds(pl.multiple_of(i * 128, 128), 128)
        z1t[:, at] = acc[at, :].T
        return carry
    lax.fori_loop(0, ROWS // 128, turn, 0)
    acc[...] = jnp.zeros_like(acc)

    def pass2(c, carry):
        gather_events(copies2, c)
        k, h = block_half(c)
        ymask[:C_PAD, :] = masked(y2all, k, h)
        g = c + CHUNKS
        fetch(g).wait()
        acc[:, :C_PAD] += lax.dot_general(abuf[lax.rem(g, SLOTS)], ymask[:C_PAD, :], NT, preferred_element_type=F32)
        next_fetch(g)
        return carry
    lax.fori_loop(0, CHUNKS, pass2, 0)

    def turn2(i, carry):
        at = pl.ds(pl.multiple_of(i * 128, 128), 128)
        z2t[:, at] = acc[at, :].T[:C_PAD]
        return carry
    lax.fori_loop(0, ROWS // 128, turn2, 0)
    for copy in count_copies:
        copy.wait_recv()
    label_count = cnt[0, 0:1, 0:1]
    for k in range(1, DEVICES):
        label_count = label_count + cnt[k, 0:1, 0:1]
    loss = jnp.zeros((1, 1), F32)
    for q in range(4):
        at = pl.ds(q * QUART, QUART)
        z = z2t[:, at]
        row = lax.broadcasted_iota(jnp.int32, (C_PAD, QUART), 0)
        z = jnp.where(row < CLASSES, z, -jnp.inf)
        top = jnp.max(z, axis=0, keepdims=True)
        log_norm = jnp.log(jnp.sum(jnp.exp(z - top), axis=0, keepdims=True)) + top
        hot = row == labels[:, at]
        picked = jnp.sum(jnp.where(hot, z, 0.0), axis=0, keepdims=True)
        w = mask[:, at].astype(F32)
        loss = loss + jnp.sum(w * (log_norm - picked), axis=1, keepdims=True)
        prob = jnp.exp(z - log_norm)
        lhs1[:, at] = ((prob - hot.astype(F32)) * (w / label_count)).astype(BF16)

    def scatter_copies(p, r, f, ix):
        def half(k, h):
            return p.at[k, :, pl.ds(h * HALF, HALF)]

        def quart(k, q):
            return p.at[k, :, pl.ds(q * QUART, QUART)]

        copies = {}
        for h in range(2):
            even, odd = 2 * h, 2 * h + 1
            for k in (7, 5, 3, 1):
                copies['core', k, h] = remote(half(k, h), r.at[k // 2, h], 1)
            copies['xy', h] = remote(quart(6, even), f.at[0, h], 2)
            copies['yx', h] = remote(quart(6, odd), f.at[1, h], 4)
            copies['y raw', h] = remote(quart(4, odd), ix.at[1, odd], 4)
            copies['x raw', h] = remote(quart(2, even), ix.at[0, even], 2)
            copies['y', h] = remote(quart(4, even), ix.at[1, even], 4)
            copies['x', h] = remote(quart(2, odd), ix.at[0, odd], 2)
        return copies

    def scatter_events(copies, p, r, f, c, pass_on):
        sends = {6: ('xy', 'yx'), 4: ('y raw',), 2: ('x raw',), 0: ()}
        for q in range(4):
            for h in range(2):
                k = 6 - 2 * q

                @pl.when(c == 4 * q + 2 * h)
                def _(k=k, h=h):
                    copies['core', k + 1, h].start()

                @pl.when(c == 4 * q + 2 * h + 1)
                def _(k=k, h=h):
                    at = pl.ds(h * HALF, HALF)
                    copies['core', k + 1, h].wait_recv()
                    p[k, :, at] = p[k, :, at] + r[k // 2, h]
                    for name in sends[k]:
                        copies[name, h].start()

        for h in range(2):
            @pl.when(c == pass_on[h])
            def _(h=h):
                even, odd = pl.ds(2 * h * QUART, QUART), pl.ds((2 * h + 1) * QUART, QUART)
                copies['xy', h].wait_recv()
                p[4, :, even] = p[4, :, even] + f[0, h]
                copies['y', h].start()
                copies['yx', h].wait_recv()
                p[2, :, odd] = p[2, :, odd] + f[1, h]
                copies['x', h].start()

    def scatter_result(copies, p, ix, q):
        h = q // 2
        for name in (('y', 'x raw') if q % 2 == 0 else ('y raw', 'x')):
            copies[name, h].wait_recv()
        return (p[0, :, pl.ds(q * QUART, QUART)] + ix[0, q] + ix[1, q]).astype(BF16)

    copies3 = scatter_copies(pa, ra, fa, ia)

    def pass3(c, carry):
        g = c + 2 * CHUNKS
        k, h = block_half(g)
        cols = pl.ds(pl.multiple_of(h * HALF, HALF), HALF)
        fetch(g).wait()
        part = jnp.dot(lhs1[...], abuf[lax.rem(g, SLOTS)], preferred_element_type=F32)
        pa[k, :, cols] = part * mask_value(k)
        next_fetch(g)
        scatter_events(copies3, pa, ra, fa, c, (11, 11))
        return carry
    lax.fori_loop(0, CHUNKS, pass3, 0)
    d2t = jnp.concatenate([scatter_result(copies3, pa, ia, q) for q in range(4)], axis=1)
    back = jnp.dot(wo_bf, d2t, preferred_element_type=F32)
    lhs2[...] = jnp.where(z1t[...] > 0.0, back, 0.0).astype(BF16)

    copies4 = scatter_copies(pb, rb, fb, ib)

    def pass4(c, carry):
        g = c + 3 * CHUNKS
        k, h = block_half(g)
        cols = pl.ds(pl.multiple_of(h * HALF, HALF), HALF)
        fetch(g).wait()
        part = jnp.dot(lhs2[...], abuf[lax.rem(g, SLOTS)], preferred_element_type=F32)
        pb[k, :, cols] = part * mask_value(k)
        next_fetch(g)
        scatter_events(copies4, pb, rb, fb, c, (11, 13))
        return carry
    lax.fori_loop(0, CHUNKS, pass4, 0)

    gpart[F_IN // 8 * 8:GWO_ROW, :] = jnp.zeros((8, HID), F32)
    gpart[GWO_ROW:LOSS_ROW, :] = jnp.dot(d2t, hid[...], preferred_element_type=F32)
    gpart[LOSS_ROW:SUM_ROWS, :] = jnp.broadcast_to(loss / label_count, (SUM_ROWS - LOSS_ROW, HID))
    for copy in list(copies2.values()) + count_copies + list(copies3.values()):
        copy.wait_send()
    for q in range(4):
        term = lax.dot_general(xbuf[:, q * QUART:(q + 1) * QUART], scatter_result(copies4, pb, ib, q), NT, preferred_element_type=F32)
        if q == 0:
            gpart[:F_IN, :] = term
        else:
            gpart[:F_IN, :] += term

    half_rows, quart_rows = SUM_ROWS // 2, SUM_ROWS // 4
    mine = pl.ds(pl.multiple_of(bits[0] * half_rows, 8), half_rows)
    other = pl.ds(pl.multiple_of((1 - bits[0]) * half_rows, 8), half_rows)
    swap = remote(gpart.at[other, :], gpair, 1)
    swap.start()
    swap.wait()
    gpart[mine, :] = gpart[mine, :] + gpair[...]
    quarts = [pl.ds(pl.multiple_of(bits[0] * half_rows + q * quart_rows, 8), quart_rows) for q in range(2)]
    for step, ways in enumerate(((2, 4), (4, 2))):
        copies = [remote(gpart.at[quarts[q], :], gacross.at[step, q], ways[q]) for q in range(2)]
        for copy in copies:
            copy.start()
        for q in range(2):
            copies[q].wait()
            gpart[quarts[q], :] = gpart[quarts[q], :] + gacross[step, q]
    final = remote(gpart.at[mine, :], gback, 1)
    final.start()
    for copy in copies4.values():
        copy.wait_send()
    final.wait()
    gpart[other, :] = gback[...]
    gwh_out[...] = gpart[:F_IN, :]
    gwo_out[...] = gpart[GWO_ROW:GWO_ROW + CLASSES, :]
    loss_out[...] = gpart[LOSS_ROW:LOSS_ROW + 1, 0:1]


def device_step(adj, feat, w_hidden, w_output, labels, train_mask, block_mask):
    vmem = pl.BlockSpec(memory_space=pltpu.VMEM)
    hbm = pl.BlockSpec(memory_space=pl.ANY)
    v = pltpu.VMEM
    copies = 96
    loss, gwh, gwo = pl.pallas_call(
        step_kernel,
        out_shape=(jax.ShapeDtypeStruct((1, 1), F32), jax.ShapeDtypeStruct((F_IN, HID), F32), jax.ShapeDtypeStruct((CLASSES, HID), F32)),
        in_specs=[hbm, hbm, vmem, vmem, vmem, vmem, pl.BlockSpec(memory_space=pltpu.SMEM)],
        out_specs=(vmem, vmem, vmem),
        scratch_shapes=[
            v((SLOTS, ROWS, HALF), BF16), v((F_IN, ROWS), BF16), v((ROWS, HID), F32),
            v((DEVICES, HID, ROWS), BF16), v((DEVICES, C_PAD, ROWS), BF16), v((HID, HALF), BF16), v((ROWS, HID), BF16),
            v((HID, ROWS), F32), v((C_PAD, ROWS), F32), v((128, 128), F32), v((C_PAD, ROWS), BF16), v((HID, ROWS), BF16),
            v((DEVICES, 8, 128), F32),
            v((DEVICES, C_PAD, ROWS), F32), v((4, 2, C_PAD, HALF), F32), v((2, 2, C_PAD, QUART), F32), v((2, 4, C_PAD, QUART), F32),
            v((DEVICES, HID, ROWS), F32), v((4, 2, HID, HALF), F32), v((2, 2, HID, QUART), F32), v((2, 4, HID, QUART), F32),
            v((SUM_ROWS, HID), F32), v((SUM_ROWS // 2, HID), F32), v((2, 2, SUM_ROWS // 4, HID), F32), v((SUM_ROWS // 2, HID), F32),
            pltpu.SemaphoreType.DMA((SLOTS,)), pltpu.SemaphoreType.DMA((1,)),
            pltpu.SemaphoreType.DMA((copies,)), pltpu.SemaphoreType.DMA((copies,)),
        ],
        compiler_params=pltpu.CompilerParams(collective_id=0, has_side_effects=True, vmem_limit_bytes=67043328),
        name='gcn_step',
    )(adj, feat.T, w_hidden, w_output.T, labels.reshape(1, ROWS), train_mask.reshape(1, ROWS), block_mask)
    return loss[0, 0], gwh, gwo.T


def solution(mesh):
    row_spec = P(AXIS_NAME, None)
    vec_spec = P(AXIS_NAME)
    return jax.shard_map(device_step, mesh=mesh, in_specs=(row_spec, row_spec, P(), P(), vec_spec, vec_spec, P()), out_specs=(P(), P(), P()), check_vma=False)
```

```python
import jax
import jax.numpy as jnp
from jax import lax
from jax.experimental import pallas as pl
from jax.experimental.pallas import tpu as pltpu
from jax.sharding import PartitionSpec as P

AXIS_NAME = 'nodes'
MESH = pl.DeviceIdType.MESH
F32, BF16 = jnp.float32, jnp.bfloat16
DEVICES = 8
ROWS = 2048
NODES = DEVICES * ROWS
F_IN = 602
HID = 128
CLASSES = 41
C_PAD = 48
HALF = ROWS // 2
QUART = ROWS // 4
SLOTS = 6
CHUNKS = NODES // HALF
SUM_ROWS = 672
GWO_ROW = 608
LOSS_ROW = GWO_ROW + C_PAD
NT = (((1,), (1,)), ((), ()))


def step_kernel(adj, feat, wh, wo, labels, mask, block_mask, loss_out, gwh_out, gwo_out,
                abuf, xbuf, acc, yall, y2all, ymask, hid, z1t, z2t, wpad, lhs1, lhs2, cnt,
                pa, ra, fa, ia, pb, rb, fb, ib, gpart, gpair, gacross, gback,
                asem, xsem, ssem, rsem):
    me = lax.axis_index(AXIS_NAME)
    bits = (lax.rem(me, 2), lax.rem(me // 2, 2), me // 4)

    def partner(k):
        return lax.rem(bits[0] + k, 2) + 2 * lax.rem(bits[1] + k // 2, 2) + 4 * lax.rem(bits[2] + k // 4, 2)

    peers = [partner(k) for k in range(DEVICES)]

    def block_quart(g, i):
        back = lax.div(g, 2 * CHUNKS)
        c = lax.rem(g, CHUNKS)
        q, r = lax.div(c, 4), lax.rem(c, 4)
        mid = lax.div(q * (3 - q), 2)
        last = lax.div(q, 3)
        pair, odd = lax.div(c, 2), lax.rem(c, 2)
        forth_k = mid * (2 + odd + 2 * i) + (1 - mid) * (last * (6 + odd) + (1 - last) * pair)
        forth_q = mid * (pair - 2) + (1 - mid) * (2 * (last * (pair - 6) + (1 - last) * odd) + i)
        back_k, back_h = mid * (5 - r) + (1 - mid) * (7 - 6 * last - odd), mid * (q - 1) + (1 - mid) * lax.div(r, 2)
        return back * back_k + (1 - back) * forth_k, back * (2 * back_h + i) + (1 - back) * forth_q

    class Fetch:
        def __init__(self, g):
            slot = lax.rem(g, SLOTS)
            self.pieces = []
            for i in range(2):
                k, q = block_quart(g, i)
                col = pl.multiple_of(partner(k) * ROWS + q * QUART, QUART)
                self.pieces.append(pltpu.make_async_copy(adj.at[:, pl.ds(col, QUART)], abuf.at[slot, :, pl.ds(i * QUART, QUART)], asem.at[slot, i]))

        def start(self):
            for piece in self.pieces:
                piece.start()

        def wait(self):
            for piece in self.pieces:
                piece.wait()

    fetch = Fetch

    used = [0]

    def remote(src, dst, k):
        i = used[0]
        used[0] += 1
        return pltpu.make_async_remote_copy(src_ref=src, dst_ref=dst, send_sem=ssem.at[i], recv_sem=rsem.at[i],
                                            device_id=(peers[k],), device_id_type=MESH)

    xcopy = pltpu.make_async_copy(feat, xbuf, xsem.at[0])
    xcopy.start()
    fetch(jnp.int32(0)).start()
    barrier = pltpu.get_barrier_semaphore()
    for k in range(1, DEVICES):
        pl.semaphore_signal(barrier, inc=1, device_id=(peers[k],), device_id_type=MESH)

    wpad[...] = jnp.zeros_like(wpad)
    wpad[:CLASSES, :] = wo[...]
    wot_bf = wpad[:C_PAD, :].astype(BF16)
    wo_bf = wpad[...].T[:, :C_PAD].astype(BF16)
    wh_t = wh[...].T.astype(BF16)
    weight = mask[...].astype(F32)
    cnt[0] = jnp.broadcast_to(jnp.sum(weight, axis=1, keepdims=True), (8, 128))
    xcopy.wait()
    for g in range(1, SLOTS):
        fetch(jnp.int32(g)).start()
    yall[0] = jnp.dot(wh_t, xbuf[...], preferred_element_type=F32).astype(BF16)
    pl.semaphore_wait(barrier, DEVICES - 1)

    def gather_copies(y):
        def half(k, h):
            return y.at[k, :, pl.ds(h * HALF, HALF)]

        def quart(k, q):
            return y.at[k, :, pl.ds(q * QUART, QUART)]

        copies = {'own': remote(y.at[0], y.at[1], 1)}
        for q in range(4):
            copies['x', q] = remote(quart(0, q), quart(2, q), 2)
            copies['y', q] = remote(quart(0, q), quart(4, q), 4)
            copies['x core', q] = remote(quart(2, q), quart(3, q), 1)
            copies['y core', q] = remote(quart(4, q), quart(5, q), 1)
            if q % 2 == 0:
                copies['across', q] = remote(quart(2, q), quart(6, q), 4)
            else:
                copies['across', q] = remote(quart(4, q), quart(6, q), 2)
        for h in range(2):
            copies['across core', h] = remote(half(6, h), half(7, h), 1)
        return copies

    def gather_start(copies):
        for q in range(4):
            copies['x', q].start()
            copies['y', q].start()
            if q == 0:
                copies['own'].start()

    def gather_need(copies, c):
        if c == 2:
            copies['own'].wait_recv()
        if 4 <= c < 12:
            q = (c - 4) // 2
            if c % 2 == 0:
                copies['x', q].wait_recv()
                if q % 2 == 0:
                    copies['across', q].start()
                copies['x core', q].start()
                copies['y', q].wait_recv()
                if q % 2 == 1:
                    copies['across', q].start()
                copies['y core', q].start()
            else:
                copies['x core', q].wait_recv()
                copies['y core', q].wait_recv()
        if c >= 12:
            h = (c - 12) // 2
            if c % 2 == 0:
                copies['across', 2 * h].wait_recv()
                copies['across', 2 * h + 1].wait_recv()
                copies['across core', h].start()
            else:
                copies['across core', h].wait_recv()

    def mask_value(k):
        return block_mask[me, partner(k)].astype(F32)

    def next_fetch(g):
        @pl.when(g + SLOTS < 4 * CHUNKS)
        def _():
            fetch(g + SLOTS).start()

    def forward_pass(copies, y, first, segments):
        width = y.shape[1]
        for begin, per_step, steps in segments:
            def step(i, carry, begin=begin, per_step=per_step, steps=steps):
                for at in range(steps):
                    needs = [begin + at * per_step + j for j in range(per_step)]
                    if any(c == 2 or c >= 4 for c in needs):
                        @pl.when(i == at)
                        def _(needs=needs):
                            for c in needs:
                                gather_need(copies, c)
                total = None
                for j in range(per_step):
                    c = begin + i * per_step + j
                    for part in range(2):
                        k, q = block_quart(c, part)
                        cols = pl.ds(pl.multiple_of(q * QUART, QUART), QUART)
                        ymask[:width, (2 * j + part) * QUART:(2 * j + part + 1) * QUART] = (y[k, :, cols].astype(F32) * mask_value(k)).astype(BF16)
                for j in range(per_step):
                    fetch(first + begin + i * per_step + j).wait()
                for j in range(per_step):
                    g = first + begin + i * per_step + j
                    term = lax.dot_general(abuf[lax.rem(g, SLOTS)], ymask[:width, j * HALF:(j + 1) * HALF], NT, preferred_element_type=F32)
                    total = term if total is None else total + term
                acc[:, :width] += total
                for j in range(per_step):
                    next_fetch(first + begin + i * per_step + j)
                return carry
            lax.fori_loop(0, steps, step, 0)

    copies1 = gather_copies(yall)
    gather_start(copies1)
    acc[...] = jnp.zeros_like(acc)
    forward_pass(copies1, yall, 0, ((0, 2, 2), (4, 1, 1), (5, 2, 3), (11, 1, 5)))

    hid[...] = jnp.maximum(acc[...], 0.0).astype(BF16)
    y2all[0] = lax.dot_general(wot_bf, hid[...], NT, preferred_element_type=F32).astype(BF16)

    copies2 = gather_copies(y2all)
    gather_start(copies2)
    count_copies = [remote(cnt.at[0], cnt.at[k], k) for k in range(1, DEVICES)]
    for copy in count_copies:
        copy.start()
    for copy in copies1.values():
        copy.wait_send()

    def turn(i, carry):
        at = pl.ds(pl.multiple_of(i * 128, 128), 128)
        z1t[:, at] = acc[at, :].T
        return carry
    lax.fori_loop(0, ROWS // 128, turn, 0)
    acc[...] = jnp.zeros_like(acc)

    forward_pass(copies2, y2all, CHUNKS, ((0, 2, 2), (4, 1, 1), (5, 2, 5), (15, 1, 1)))

    def turn2(i, carry):
        at = pl.ds(pl.multiple_of(i * 128, 128), 128)
        z2t[:, at] = acc[at, :].T[:C_PAD]
        return carry
    lax.fori_loop(0, ROWS // 128, turn2, 0)
    for copy in count_copies:
        copy.wait_recv()
    label_count = cnt[0, 0:1, 0:1]
    for k in range(1, DEVICES):
        label_count = label_count + cnt[k, 0:1, 0:1]
    loss = jnp.zeros((1, 1), F32)
    for q in range(4):
        at = pl.ds(q * QUART, QUART)
        z = z2t[:, at]
        row = lax.broadcasted_iota(jnp.int32, (C_PAD, QUART), 0)
        z = jnp.where(row < CLASSES, z, -jnp.inf)
        top = jnp.max(z, axis=0, keepdims=True)
        log_norm = jnp.log(jnp.sum(jnp.exp(z - top), axis=0, keepdims=True)) + top
        hot = row == labels[:, at]
        picked = jnp.sum(jnp.where(hot, z, 0.0), axis=0, keepdims=True)
        w = mask[:, at].astype(F32)
        loss = loss + jnp.sum(w * (log_norm - picked), axis=1, keepdims=True)
        prob = jnp.exp(z - log_norm)
        lhs1[:, at] = ((prob - hot.astype(F32)) * (w / label_count)).astype(BF16)

    def scatter_copies(p, r, f, ix):
        def half(k, h):
            return p.at[k, :, pl.ds(h * HALF, HALF)]

        def quart(k, q):
            return p.at[k, :, pl.ds(q * QUART, QUART)]

        copies = {}
        for h in range(2):
            even, odd = 2 * h, 2 * h + 1
            for k in (7, 5, 3, 1):
                copies['core', k, h] = remote(half(k, h), r.at[k // 2, h], 1)
            copies['xy', h] = remote(quart(6, even), f.at[0, h], 2)
            copies['yx', h] = remote(quart(6, odd), f.at[1, h], 4)
            copies['y raw', h] = remote(quart(4, odd), ix.at[1, odd], 4)
            copies['x raw', h] = remote(quart(2, even), ix.at[0, even], 2)
            copies['y', h] = remote(quart(4, even), ix.at[1, even], 4)
            copies['x', h] = remote(quart(2, odd), ix.at[0, odd], 2)
        return copies

    def scatter_events(copies, p, r, f, c, pass_on):
        sends = {6: ('xy', 'yx'), 4: ('y raw',), 2: ('x raw',), 0: ()}
        order = [(7, 0), (6, 0), (7, 1), (6, 1)] + [(k, h) for h in range(2) for k in (5, 4, 3, 2)] + [(1, 0), (0, 0), (1, 1), (0, 1)]
        for at, (k, h) in enumerate(order):
            @pl.when(c == at)
            def _(at=at, k=k, h=h):
                if k % 2 == 1:
                    copies['core', k, h].start()
                else:
                    cols = pl.ds(h * HALF, HALF)
                    copies['core', k + 1, h].wait_recv()
                    p[k, :, cols] = p[k, :, cols] + r[k // 2, h]
                    for name in sends[k]:
                        copies[name, h].start()
                for way, h2 in pass_on.get(at, ()):
                    if way == 'y':
                        even = pl.ds(2 * h2 * QUART, QUART)
                        copies['xy', h2].wait_recv()
                        p[4, :, even] = p[4, :, even] + f[0, h2]
                    else:
                        odd = pl.ds((2 * h2 + 1) * QUART, QUART)
                        copies['yx', h2].wait_recv()
                        p[2, :, odd] = p[2, :, odd] + f[1, h2]
                    copies[way, h2].start()

    def scatter_result(copies, p, ix, q):
        h = q // 2
        for name in (('y', 'x raw') if q % 2 == 0 else ('y raw', 'x')):
            copies[name, h].wait_recv()
        return (p[0, :, pl.ds(q * QUART, QUART)] + ix[0, q] + ix[1, q]).astype(BF16)

    copies3 = scatter_copies(pa, ra, fa, ia)

    def pass3(c, carry):
        g = c + 2 * CHUNKS
        k, q = block_quart(g, 0)
        cols = pl.ds(pl.multiple_of(q * QUART, HALF), HALF)
        fetch(g).wait()
        part = jnp.dot(lhs1[...], abuf[lax.rem(g, SLOTS)], preferred_element_type=F32)
        pa[k, :, cols] = part * mask_value(k)
        next_fetch(g)
        scatter_events(copies3, pa, ra, fa, c, {6: (('y', 0),), 7: (('x', 0),), 9: (('y', 1),), 11: (('x', 1),)})
        return carry
    lax.fori_loop(0, CHUNKS, pass3, 0)
    d2t = jnp.concatenate([scatter_result(copies3, pa, ia, q) for q in range(4)], axis=1)
    back = jnp.dot(wo_bf, d2t, preferred_element_type=F32)
    lhs2[...] = jnp.where(z1t[...] > 0.0, back, 0.0).astype(BF16)

    copies4 = scatter_copies(pb, rb, fb, ib)

    def pass4(c, carry):
        g = c + 3 * CHUNKS
        k, q = block_quart(g, 0)
        cols = pl.ds(pl.multiple_of(q * QUART, HALF), HALF)
        fetch(g).wait()
        part = jnp.dot(lhs2[...], abuf[lax.rem(g, SLOTS)], preferred_element_type=F32)
        pb[k, :, cols] = part * mask_value(k)
        next_fetch(g)
        scatter_events(copies4, pb, rb, fb, c, {9: (('y', 0),), 10: (('x', 0),), 13: (('y', 1), ('x', 1))})
        return carry
    lax.fori_loop(0, CHUNKS, pass4, 0)

    gpart[F_IN // 8 * 8:GWO_ROW, :] = jnp.zeros((8, HID), F32)
    gpart[GWO_ROW:LOSS_ROW, :] = jnp.dot(d2t, hid[...], preferred_element_type=F32)
    gpart[LOSS_ROW:SUM_ROWS, :] = jnp.broadcast_to(loss / label_count, (SUM_ROWS - LOSS_ROW, HID))
    for copy in list(copies2.values()) + count_copies + list(copies3.values()):
        copy.wait_send()
    for q in range(4):
        term = lax.dot_general(xbuf[:, q * QUART:(q + 1) * QUART], scatter_result(copies4, pb, ib, q), NT, preferred_element_type=F32)
        if q == 0:
            gpart[:F_IN, :] = term
        else:
            gpart[:F_IN, :] += term

    half_rows, quart_rows = SUM_ROWS // 2, SUM_ROWS // 4
    mine = pl.ds(pl.multiple_of(bits[0] * half_rows, 8), half_rows)
    other = pl.ds(pl.multiple_of((1 - bits[0]) * half_rows, 8), half_rows)
    swap = remote(gpart.at[other, :], gpair, 1)
    swap.start()
    swap.wait()
    gpart[mine, :] = gpart[mine, :] + gpair[...]
    quarts = [pl.ds(pl.multiple_of(bits[0] * half_rows + q * quart_rows, 8), quart_rows) for q in range(2)]
    for step, ways in enumerate(((2, 4), (4, 2))):
        copies = [remote(gpart.at[quarts[q], :], gacross.at[step, q], ways[q]) for q in range(2)]
        for copy in copies:
            copy.start()
        for q in range(2):
            copies[q].wait()
            gpart[quarts[q], :] = gpart[quarts[q], :] + gacross[step, q]
    final = remote(gpart.at[mine, :], gback, 1)
    final.start()
    for copy in copies4.values():
        copy.wait_send()
    final.wait()
    gpart[other, :] = gback[...]
    gwh_out[...] = gpart[:F_IN, :]
    gwo_out[...] = gpart[GWO_ROW:GWO_ROW + CLASSES, :]
    loss_out[...] = gpart[LOSS_ROW:LOSS_ROW + 1, 0:1]


def device_step(adj, feat, w_hidden, w_output, labels, train_mask, block_mask):
    vmem = pl.BlockSpec(memory_space=pltpu.VMEM)
    hbm = pl.BlockSpec(memory_space=pl.ANY)
    v = pltpu.VMEM
    copies = 112
    loss, gwh, gwo = pl.pallas_call(
        step_kernel,
        out_shape=(jax.ShapeDtypeStruct((1, 1), F32), jax.ShapeDtypeStruct((F_IN, HID), F32), jax.ShapeDtypeStruct((CLASSES, HID), F32)),
        in_specs=[hbm, hbm, vmem, vmem, vmem, vmem, pl.BlockSpec(memory_space=pltpu.SMEM)],
        out_specs=(vmem, vmem, vmem),
        scratch_shapes=[
            v((SLOTS, ROWS, HALF), BF16), v((F_IN, ROWS), BF16), v((ROWS, HID), F32),
            v((DEVICES, HID, ROWS), BF16), v((DEVICES, C_PAD, ROWS), BF16), v((HID, ROWS), BF16), v((ROWS, HID), BF16),
            v((HID, ROWS), F32), v((C_PAD, ROWS), F32), v((128, 128), F32), v((C_PAD, ROWS), BF16), v((HID, ROWS), BF16),
            v((DEVICES, 8, 128), F32),
            v((DEVICES, C_PAD, ROWS), F32), v((4, 2, C_PAD, HALF), F32), v((2, 2, C_PAD, QUART), F32), v((2, 4, C_PAD, QUART), F32),
            v((DEVICES, HID, ROWS), F32), v((4, 2, HID, HALF), F32), v((2, 2, HID, QUART), F32), v((2, 4, HID, QUART), F32),
            v((SUM_ROWS, HID), F32), v((SUM_ROWS // 2, HID), F32), v((2, 2, SUM_ROWS // 4, HID), F32), v((SUM_ROWS // 2, HID), F32),
            pltpu.SemaphoreType.DMA((SLOTS, 2)), pltpu.SemaphoreType.DMA((1,)),
            pltpu.SemaphoreType.DMA((copies,)), pltpu.SemaphoreType.DMA((copies,)),
        ],
        compiler_params=pltpu.CompilerParams(collective_id=0, has_side_effects=True, vmem_limit_bytes=67043328),
        name='gcn_step',
    )(adj, feat.T, w_hidden, w_output.T, labels.reshape(1, ROWS), train_mask.reshape(1, ROWS), block_mask)
    return loss[0, 0], gwh, gwo.T


def solution(mesh):
    row_spec = P(AXIS_NAME, None)
    vec_spec = P(AXIS_NAME)
    return jax.shard_map(device_step, mesh=mesh, in_specs=(row_spec, row_spec, P(), P(), vec_spec, vec_spec, P()), out_specs=(P(), P(), P()), check_vma=False)
```

```python
import jax
import jax.numpy as jnp
from jax import lax
from jax.experimental import pallas as pl
from jax.experimental.pallas import tpu as pltpu
from jax.sharding import PartitionSpec as P

AXIS_NAME = 'nodes'
MESH = pl.DeviceIdType.MESH
F32, BF16 = jnp.float32, jnp.bfloat16
DEVICES = 8
ROWS = 2048
NODES = DEVICES * ROWS
F_IN = 602
HID = 128
CLASSES = 41
C_PAD = 48
HALF = ROWS // 2
QUART = ROWS // 4
SLOTS = 8
CHUNKS = NODES // HALF
SUM_ROWS = 672
GWO_ROW = 608
LOSS_ROW = GWO_ROW + C_PAD
NT = (((1,), (1,)), ((), ()))


def step_kernel(adj, feat, wh_in, wo_in, labels_in, mask_in, block_mask, sums_out,
                abuf, xbuf, wh, wo, labels, mask, acc, yall, y2all, ymask, hid, z1t, wpad, lhs1, lhs2, cnt,
                ra, fa, ia, pb, rb, fb, ib, gpart, gpair, gacross,
                asem, xsem, ssem, rsem):
    me = lax.axis_index(AXIS_NAME)
    bits = (lax.rem(me, 2), lax.rem(me // 2, 2), me // 4)

    def partner(k):
        return lax.rem(bits[0] + k, 2) + 2 * lax.rem(bits[1] + k // 2, 2) + 4 * lax.rem(bits[2] + k // 4, 2)

    peers = [partner(k) for k in range(DEVICES)]

    def block_quart(g, i):
        back = lax.div(g, 2 * CHUNKS)
        c = lax.rem(g, CHUNKS)
        q, r = lax.div(c, 4), lax.rem(c, 4)
        mid = lax.div(q * (3 - q), 2)
        last = lax.div(q, 3)
        pair, odd = lax.div(c, 2), lax.rem(c, 2)
        forth_k = mid * (2 + odd + 2 * i) + (1 - mid) * (last * (6 + odd) + (1 - last) * pair)
        forth_q = mid * (pair - 2) + (1 - mid) * (2 * (last * (pair - 6) + (1 - last) * odd) + i)
        back_k, back_h = mid * (5 - r) + (1 - mid) * (7 - 6 * last - odd), mid * (q - 1) + (1 - mid) * lax.div(r, 2)
        return back * back_k + (1 - back) * forth_k, back * (2 * back_h + i) + (1 - back) * forth_q

    class Fetch:
        def __init__(self, g):
            slot = lax.rem(g, SLOTS)
            self.pieces = []
            for i in range(2):
                k, q = block_quart(g, i)
                col = pl.multiple_of(partner(k) * ROWS + q * QUART, QUART)
                self.pieces.append(pltpu.make_async_copy(adj.at[:, pl.ds(col, QUART)], abuf.at[slot, :, pl.ds(i * QUART, QUART)], asem.at[slot, i]))

        def start(self):
            for piece in self.pieces:
                piece.start()

        def wait(self):
            for piece in self.pieces:
                piece.wait()

    fetch = Fetch

    used = [0]

    def remote(src, dst, k):
        i = used[0]
        used[0] += 1
        return pltpu.make_async_remote_copy(src_ref=src, dst_ref=dst, send_sem=ssem.at[i], recv_sem=rsem.at[i],
                                            device_id=(peers[k],), device_id_type=MESH)

    xcopy = pltpu.make_async_copy(feat, xbuf, xsem.at[0])
    xcopy.start()
    small = [pltpu.make_async_copy(src, dst, xsem.at[1 + i]) for i, (src, dst) in
             enumerate(((wh_in, wh), (wo_in, wo), (labels_in, labels), (mask_in, mask)))]
    for copy in small:
        copy.start()
    fetch(jnp.int32(0)).start()
    barrier = pltpu.get_barrier_semaphore()
    for k in range(1, DEVICES):
        pl.semaphore_signal(barrier, inc=1, device_id=(peers[k],), device_id_type=MESH)

    for copy in small:
        copy.wait()
    wpad[...] = jnp.zeros_like(wpad)
    wpad[:CLASSES, :] = wo[...]
    wot_bf = wpad[:C_PAD, :].astype(BF16)
    wo_bf = wpad[...].T[:, :C_PAD].astype(BF16)
    wh_t = wh[...].T.astype(BF16)
    weight = mask[...].astype(F32)
    cnt[0] = jnp.broadcast_to(jnp.sum(weight, axis=1, keepdims=True), (8, 128))
    xcopy.wait()
    for g in range(1, SLOTS - 2):
        fetch(jnp.int32(g)).start()
    yall[0] = jnp.dot(wh_t, xbuf[...], preferred_element_type=F32).astype(BF16)
    pl.semaphore_wait(barrier, DEVICES - 1)

    def gather_copies(y):
        def half(k, h):
            return y.at[k, :, pl.ds(h * HALF, HALF)]

        def quart(k, q):
            return y.at[k, :, pl.ds(q * QUART, QUART)]

        copies = {'own': remote(y.at[0], y.at[1], 1)}
        for q in range(4):
            copies['x', q] = remote(quart(0, q), quart(2, q), 2)
            copies['y', q] = remote(quart(0, q), quart(4, q), 4)
            copies['x core', q] = remote(quart(2, q), quart(3, q), 1)
            copies['y core', q] = remote(quart(4, q), quart(5, q), 1)
            if q % 2 == 0:
                copies['across', q] = remote(quart(2, q), quart(6, q), 4)
            else:
                copies['across', q] = remote(quart(4, q), quart(6, q), 2)
        for h in range(2):
            copies['across core', h] = remote(half(6, h), half(7, h), 1)
        return copies

    def gather_start(copies):
        for q in range(4):
            copies['x', q].start()
            copies['y', q].start()
            if q == 0:
                copies['own'].start()

    def gather_need(copies, c):
        if c == 2:
            copies['own'].wait_recv()
        if 4 <= c < 12:
            q = (c - 4) // 2
            if c % 2 == 0:
                copies['x', q].wait_recv()
                if q % 2 == 0:
                    copies['across', q].start()
                copies['x core', q].start()
                copies['y', q].wait_recv()
                if q % 2 == 1:
                    copies['across', q].start()
                copies['y core', q].start()
            else:
                copies['x core', q].wait_recv()
                copies['y core', q].wait_recv()
        if c >= 12:
            h = (c - 12) // 2
            if c % 2 == 0:
                copies['across', 2 * h].wait_recv()
                copies['across', 2 * h + 1].wait_recv()
                copies['across core', h].start()
            else:
                copies['across core', h].wait_recv()

    def mask_value(k):
        return block_mask[me, partner(k)].astype(F32)

    def forward_pass(copies, y, first, segments):
        width = y.shape[1]
        for begin, per_step, steps in segments:
            def step(i, carry, begin=begin, per_step=per_step, steps=steps):
                for at in range(steps):
                    needs = [begin + at * per_step + j for j in range(per_step)]
                    if any(c == 2 or c >= 4 for c in needs):
                        @pl.when(i == at)
                        def _(needs=needs):
                            for c in needs:
                                gather_need(copies, c)
                total = None
                for j in range(per_step):
                    c = begin + i * per_step + j
                    for part in range(2):
                        k, q = block_quart(c, part)
                        cols = pl.ds(pl.multiple_of(q * QUART, QUART), QUART)
                        ymask[:width, (2 * j + part) * QUART:(2 * j + part + 1) * QUART] = (y[k, :, cols].astype(F32) * mask_value(k)).astype(BF16)
                for j in range(per_step):
                    fetch(first + begin + i * per_step + j).wait()
                for j in range(per_step):
                    fetch(first + begin + i * per_step + j + SLOTS - 2).start()
                for j in range(per_step):
                    g = first + begin + i * per_step + j
                    term = lax.dot_general(abuf[lax.rem(g, SLOTS)], ymask[:width, j * HALF:(j + 1) * HALF], NT, preferred_element_type=F32)
                    total = term if total is None else total + term
                acc[:, :width] += total
                return carry
            lax.fori_loop(0, steps, step, 0)

    copies1 = gather_copies(yall)
    gather_start(copies1)
    acc[...] = jnp.zeros_like(acc)
    forward_pass(copies1, yall, 0, ((0, 2, 2), (4, 1, 1), (5, 2, 3), (11, 1, 5)))

    hid[...] = jnp.maximum(acc[...], 0.0).astype(BF16)
    y2all[0] = lax.dot_general(wot_bf, hid[...], NT, preferred_element_type=F32).astype(BF16)

    copies2 = gather_copies(y2all)
    gather_start(copies2)
    count_copies = [remote(cnt.at[0], cnt.at[k], k) for k in range(1, DEVICES)]
    for copy in count_copies:
        copy.start()
    for copy in copies1.values():
        copy.wait_send()

    def turn(i, carry):
        at = pl.ds(pl.multiple_of(i * 128, 128), 128)
        z1t[:, at] = (acc[at, :] > 0.0).astype(F32).T.astype(BF16)
        return carry
    lax.fori_loop(0, ROWS // 128, turn, 0)
    acc[...] = jnp.zeros_like(acc)

    forward_pass(copies2, y2all, CHUNKS, ((0, 2, 2), (4, 1, 1), (5, 2, 5), (15, 1, 1)))

    def turn2(i, carry):
        at = pl.ds(pl.multiple_of(i * 128, 128), 128)
        pb[0, :C_PAD, at] = acc[at, :].T[:C_PAD]
        return carry
    lax.fori_loop(0, ROWS // 128, turn2, 0)
    for copy in count_copies:
        copy.wait_recv()
    label_count = cnt[0, 0:1, 0:1]
    for k in range(1, DEVICES):
        label_count = label_count + cnt[k, 0:1, 0:1]
    loss = jnp.zeros((1, 1), F32)
    for q in range(4):
        at = pl.ds(q * QUART, QUART)
        z = pb[0, :C_PAD, at]
        row = lax.broadcasted_iota(jnp.int32, (C_PAD, QUART), 0)
        z = jnp.where(row < CLASSES, z, -jnp.inf)
        top = jnp.max(z, axis=0, keepdims=True)
        log_norm = jnp.log(jnp.sum(jnp.exp(z - top), axis=0, keepdims=True)) + top
        hot = row == labels[:, at]
        picked = jnp.sum(jnp.where(hot, z, 0.0), axis=0, keepdims=True)
        w = mask[:, at].astype(F32)
        loss = loss + jnp.sum(w * (log_norm - picked), axis=1, keepdims=True)
        prob = jnp.exp(z - log_norm)
        lhs1[:, at] = ((prob - hot.astype(F32)) * (w / label_count)).astype(BF16)

    def scatter_copies(p, r, f, ix):
        def half(k, h):
            return p.at[k, :, pl.ds(h * HALF, HALF)]

        def quart(k, q):
            return p.at[k, :, pl.ds(q * QUART, QUART)]

        copies = {}
        for h in range(2):
            even, odd = 2 * h, 2 * h + 1
            for k in (7, 5, 3, 1):
                copies['core', k, h] = remote(half(k, h), r.at[k // 2, h], 1)
            copies['xy', h] = remote(quart(6, even), f.at[0, h], 2)
            copies['yx', h] = remote(quart(6, odd), f.at[1, h], 4)
            copies['y raw', h] = remote(quart(4, odd), ix.at[1, odd], 4)
            copies['x raw', h] = remote(quart(2, even), ix.at[0, even], 2)
            copies['y', h] = remote(quart(4, even), ix.at[1, even], 4)
            copies['x', h] = remote(quart(2, odd), ix.at[0, odd], 2)
        return copies

    def scatter_events(copies, p, r, f, c, pass_on):
        sends = {6: ('xy', 'yx'), 4: ('y raw',), 2: ('x raw',), 0: ()}
        order = [(7, 0), (6, 0), (7, 1), (6, 1)] + [(k, h) for h in range(2) for k in (5, 4, 3, 2)] + [(1, 0), (0, 0), (1, 1), (0, 1)]
        for at, (k, h) in enumerate(order):
            @pl.when(c == at)
            def _(at=at, k=k, h=h):
                if k % 2 == 1:
                    copies['core', k, h].start()
                else:
                    cols = pl.ds(h * HALF, HALF)
                    copies['core', k + 1, h].wait_recv()
                    p[k, :, cols] = p[k, :, cols] + r[k // 2, h]
                    for name in sends[k]:
                        copies[name, h].start()
                for way, h2 in pass_on.get(at, ()):
                    if way == 'y':
                        even = pl.ds(2 * h2 * QUART, QUART)
                        copies['xy', h2].wait_recv()
                        p[4, :, even] = p[4, :, even] + f[0, h2]
                    else:
                        odd = pl.ds((2 * h2 + 1) * QUART, QUART)
                        copies['yx', h2].wait_recv()
                        p[2, :, odd] = p[2, :, odd] + f[1, h2]
                    copies[way, h2].start()

    def scatter_result(copies, p, ix, q):
        h = q // 2
        for name in (('y', 'x raw') if q % 2 == 0 else ('y raw', 'x')):
            copies[name, h].wait_recv()
        return (p[0, :, pl.ds(q * QUART, QUART)] + ix[0, q] + ix[1, q]).astype(BF16)

    pa = pb.at[:, pl.ds(0, C_PAD), :]
    copies3 = scatter_copies(pa, ra, fa, ia)

    def pass3(c, carry):
        g = c + 2 * CHUNKS
        k, q = block_quart(g, 0)
        cols = pl.ds(pl.multiple_of(q * QUART, HALF), HALF)
        fetch(g).wait()
        fetch(g + SLOTS - 2).start()
        part = jnp.dot(lhs1[...], abuf[lax.rem(g, SLOTS)], preferred_element_type=F32)
        pa[k, :, cols] = part * mask_value(k)
        scatter_events(copies3, pa, ra, fa, c, {6: (('y', 0),), 7: (('x', 0),), 9: (('y', 1),), 11: (('x', 1),)})
        return carry
    lax.fori_loop(0, CHUNKS, pass3, 0)
    d2t = jnp.concatenate([scatter_result(copies3, pa, ia, q) for q in range(4)], axis=1)
    back = jnp.dot(wo_bf, d2t, preferred_element_type=F32)
    lhs2[...] = jnp.where(z1t[...].astype(F32) > 0.0, back, 0.0).astype(BF16)

    for copy in copies3.values():
        copy.wait_send()

    copies4 = scatter_copies(pb, rb, fb, ib)

    def pass4(c, carry):
        g = c + 3 * CHUNKS
        k, q = block_quart(g, 0)
        cols = pl.ds(pl.multiple_of(q * QUART, HALF), HALF)
        fetch(g).wait()

        @pl.when(g + SLOTS - 2 < 4 * CHUNKS)
        def _():
            fetch(g + SLOTS - 2).start()
        part = jnp.dot(lhs2[...], abuf[lax.rem(g, SLOTS)], preferred_element_type=F32)
        pb[k, :, cols] = part * mask_value(k)
        scatter_events(copies4, pb, rb, fb, c, {9: (('y', 0),), 10: (('x', 0),), 13: (('y', 1), ('x', 1))})
        return carry
    lax.fori_loop(0, CHUNKS, pass4, 0)

    gpart[F_IN // 8 * 8:GWO_ROW, :] = jnp.zeros((8, HID), F32)
    gpart[GWO_ROW:LOSS_ROW, :] = jnp.dot(d2t, hid[...], preferred_element_type=F32)
    gpart[LOSS_ROW:SUM_ROWS, :] = jnp.broadcast_to(loss / label_count, (SUM_ROWS - LOSS_ROW, HID))
    for copy in list(copies2.values()) + count_copies:
        copy.wait_send()
    for q in range(4):
        term = lax.dot_general(xbuf[:, q * QUART:(q + 1) * QUART], scatter_result(copies4, pb, ib, q), NT, preferred_element_type=F32)
        if q == 0:
            gpart[:F_IN, :] = term
        else:
            gpart[:F_IN, :] += term

    half_rows, quart_rows = SUM_ROWS // 2, SUM_ROWS // 4
    mine = pl.ds(pl.multiple_of(bits[0] * half_rows, 8), half_rows)
    other = pl.ds(pl.multiple_of((1 - bits[0]) * half_rows, 8), half_rows)
    swap = remote(gpart.at[other, :], gpair, 1)
    swap.start()
    swap.wait()
    gpart[mine, :] = gpart[mine, :] + gpair[...]
    quarts = [pl.ds(pl.multiple_of(bits[0] * half_rows + q * quart_rows, 8), quart_rows) for q in range(2)]
    for step, ways in enumerate(((2, 4), (4, 2))):
        copies = [remote(gpart.at[quarts[q], :], gacross.at[step, q], ways[q]) for q in range(2)]
        for copy in copies:
            copy.start()
        for q in range(2):
            copies[q].wait()
            gpart[quarts[q], :] = gpart[quarts[q], :] + gacross[step, q]
    final = remote(gpart.at[mine, :], sums_out.at[mine, :], 1)
    final.start()
    keep = pltpu.make_async_copy(gpart.at[mine, :], sums_out.at[mine, :], xsem.at[0])
    keep.start()
    for copy in copies4.values():
        copy.wait_send()
    keep.wait()
    final.wait()


def cut_kernel(sums, loss_out, gwh_out, gwo_out):
    gwh_out[...] = sums[:F_IN, :]
    gwo_out[...] = sums[GWO_ROW:GWO_ROW + CLASSES, :]
    loss_out[...] = sums[LOSS_ROW:LOSS_ROW + 1, 0:1]


def device_step(adj, feat, w_hidden, w_output, labels, train_mask, block_mask):
    vmem = pl.BlockSpec(memory_space=pltpu.VMEM)
    hbm = pl.BlockSpec(memory_space=pl.ANY)
    v = pltpu.VMEM
    copies = 112
    sums = pl.pallas_call(
        step_kernel,
        out_shape=jax.ShapeDtypeStruct((SUM_ROWS, HID), F32),
        in_specs=[hbm] * 6 + [pl.BlockSpec(memory_space=pltpu.SMEM)],
        out_specs=hbm,
        scratch_shapes=[
            v((SLOTS, ROWS, HALF), BF16), v((F_IN, ROWS), BF16), v((F_IN, HID), F32), v((CLASSES, HID), F32), v((1, ROWS), jnp.int32), v((1, ROWS), jnp.int32), v((ROWS, HID), F32),
            v((DEVICES, HID, ROWS), BF16), v((DEVICES, C_PAD, ROWS), BF16), v((HID, ROWS), BF16), v((ROWS, HID), BF16),
            v((HID, ROWS), BF16), v((128, 128), F32), v((C_PAD, ROWS), BF16), v((HID, ROWS), BF16),
            v((DEVICES, 8, 128), F32),
            v((4, 2, C_PAD, HALF), F32), v((2, 2, C_PAD, QUART), F32), v((2, 4, C_PAD, QUART), F32),
            v((DEVICES, HID, ROWS), F32), v((4, 2, HID, HALF), F32), v((2, 2, HID, QUART), F32), v((2, 4, HID, QUART), F32),
            v((SUM_ROWS, HID), F32), v((SUM_ROWS // 2, HID), F32), v((2, 2, SUM_ROWS // 4, HID), F32),
            pltpu.SemaphoreType.DMA((SLOTS, 2)), pltpu.SemaphoreType.DMA((5,)),
            pltpu.SemaphoreType.DMA((copies,)), pltpu.SemaphoreType.DMA((copies,)),
        ],
        compiler_params=pltpu.CompilerParams(collective_id=0, has_side_effects=True, vmem_limit_bytes=67043328),
        name='gcn_step',
    )(adj, feat.T, w_hidden, w_output.T, labels.reshape(1, ROWS), train_mask.reshape(1, ROWS), block_mask)
    loss, gwh, gwo = pl.pallas_call(
        cut_kernel,
        out_shape=(jax.ShapeDtypeStruct((1, 1), F32), jax.ShapeDtypeStruct((F_IN, HID), F32), jax.ShapeDtypeStruct((CLASSES, HID), F32)),
        in_specs=[vmem],
        out_specs=(vmem, vmem, vmem),
        compiler_params=pltpu.CompilerParams(vmem_limit_bytes=4 * 2**20),
        name='cut',
    )(sums)
    return loss[0, 0], gwh, gwo.T


def solution(mesh):
    row_spec = P(AXIS_NAME, None)
    vec_spec = P(AXIS_NAME)
    return jax.shard_map(device_step, mesh=mesh, in_specs=(row_spec, row_spec, P(), P(), vec_spec, vec_spec, P()), out_specs=(P(), P(), P()), check_vma=False)
```

```python
import jax
import jax.numpy as jnp
from jax import lax
from jax.experimental import pallas as pl
from jax.experimental.pallas import tpu as pltpu
from jax.sharding import PartitionSpec as P

AXIS_NAME = 'nodes'
MESH = pl.DeviceIdType.MESH
F32, BF16 = jnp.float32, jnp.bfloat16
DEVICES = 8
ROWS = 2048
NODES = DEVICES * ROWS
F_IN = 602
HID = 128
CLASSES = 41
C_PAD = 48
HALF = ROWS // 2
QUART = ROWS // 4
SLOTS = 8
CHUNKS = NODES // HALF
SUM_ROWS = 672
GWO_ROW = 608
LOSS_ROW = GWO_ROW + C_PAD
NT = (((1,), (1,)), ((), ()))


def step_kernel(adj, feat, wh_in, wo_in, labels_in, mask_in, block_mask, sums_out,
                abuf, xbuf, wh, wo, labels, mask, acc, yall, y2all, ymask, hid, hidt, wpad, lhs, cnt,
                ra, fa, ia, pb, rb, fb, ib, gpart, gpair, gacross,
                asem, xsem, ssem, rsem):
    me = lax.axis_index(AXIS_NAME)
    bits = (lax.rem(me, 2), lax.rem(me // 2, 2), me // 4)

    def partner(k):
        return lax.rem(bits[0] + k, 2) + 2 * lax.rem(bits[1] + k // 2, 2) + 4 * lax.rem(bits[2] + k // 4, 2)

    peers = [partner(k) for k in range(DEVICES)]

    def block_quart(g, i):
        back = lax.div(g, 2 * CHUNKS)
        c = lax.rem(g, CHUNKS)
        q, r = lax.div(c, 4), lax.rem(c, 4)
        mid = lax.div(q * (3 - q), 2)
        last = lax.div(q, 3)
        pair, odd = lax.div(c, 2), lax.rem(c, 2)
        forth_k = mid * (2 + odd + 2 * i) + (1 - mid) * (last * (6 + odd) + (1 - last) * pair)
        forth_q = mid * (pair - 2) + (1 - mid) * (2 * (last * (pair - 6) + (1 - last) * odd) + i)
        back_k, back_h = mid * (5 - r) + (1 - mid) * (7 - 6 * last - odd), mid * (q - 1) + (1 - mid) * lax.div(r, 2)
        return back * back_k + (1 - back) * forth_k, back * (2 * back_h + i) + (1 - back) * forth_q

    class Fetch:
        def __init__(self, g):
            slot = lax.rem(g, SLOTS)
            self.pieces = []
            for i in range(2):
                k, q = block_quart(g, i)
                col = pl.multiple_of(partner(k) * ROWS + q * QUART, QUART)
                self.pieces.append(pltpu.make_async_copy(adj.at[:, pl.ds(col, QUART)], abuf.at[slot, :, pl.ds(i * QUART, QUART)], asem.at[slot, i]))

        def start(self):
            for piece in self.pieces:
                piece.start()

        def wait(self):
            for piece in self.pieces:
                piece.wait()

    fetch = Fetch

    def remote(src, dst, k, send, recv):
        return pltpu.make_async_remote_copy(src_ref=src, dst_ref=dst, send_sem=ssem.at[send], recv_sem=rsem.at[recv],
                                            device_id=(peers[k],), device_id_type=MESH)

    xcopy = pltpu.make_async_copy(feat, xbuf, xsem.at[0])
    xcopy.start()
    small = [pltpu.make_async_copy(src, dst, xsem.at[1 + i]) for i, (src, dst) in
             enumerate(((wh_in, wh), (wo_in, wo), (labels_in, labels), (mask_in, mask)))]
    for copy in small:
        copy.start()
    fetch(jnp.int32(0)).start()
    fetch(jnp.int32(1)).start()
    barrier = pltpu.get_barrier_semaphore()
    for k in range(1, DEVICES):
        pl.semaphore_signal(barrier, inc=1, device_id=(peers[k],), device_id_type=MESH)

    for copy in small:
        copy.wait()
    wpad[...] = jnp.zeros_like(wpad)
    wpad[:CLASSES, :] = wo[...]
    wot_bf = wpad[:C_PAD, :].astype(BF16)
    wo_bf = wpad[...].T[:, :C_PAD].astype(BF16)
    wh_t = wh[...].T.astype(BF16)
    weight = mask[...].astype(F32)
    cnt[0] = jnp.broadcast_to(jnp.sum(weight, axis=1, keepdims=True), (8, 128))
    xcopy.wait()
    for g in range(2, SLOTS - 2):
        fetch(jnp.int32(g)).start()
    yall[0] = jnp.dot(wh_t, xbuf[...], preferred_element_type=F32).astype(BF16)
    pl.semaphore_wait(barrier, DEVICES - 1)

    def gather_copies(y, send, recv):
        def half(k, h):
            return y.at[k, :, pl.ds(h * HALF, HALF)]

        def quart(k, q):
            return y.at[k, :, pl.ds(q * QUART, QUART)]

        copies = {'own': remote(y.at[0], y.at[1], 1, send, recv)}
        for q in range(4):
            copies['x', q] = remote(quart(0, q), quart(2, q), 2, send, recv + 1 + q)
            copies['y', q] = remote(quart(0, q), quart(4, q), 4, send, recv + 1 + q)
            copies['x core', q] = remote(quart(2, q), quart(3, q), 1, send, recv + 5 + q)
            copies['y core', q] = remote(quart(4, q), quart(5, q), 1, send, recv + 5 + q)
            copies['both', q] = remote(half(0, 0), half(0, 0), 2, send, recv + 1 + q)
            copies['both core', q] = remote(half(0, 0), half(0, 0), 1, send, recv + 5 + q)
            if q % 2 == 0:
                copies['across', q] = remote(quart(2, q), quart(6, q), 4, send, recv + 9 + q // 2)
            else:
                copies['across', q] = remote(quart(4, q), quart(6, q), 2, send, recv + 9 + q // 2)
        for h in range(2):
            copies['across both', h] = remote(half(0, 0), half(0, 0), 2, send, recv + 9 + h)
            copies['across core', h] = remote(half(6, h), half(7, h), 1, send, recv + 11 + h)
        copies['sent'] = remote(y.at[pl.ds(0, 7)], y.at[pl.ds(0, 7)], 1, send, recv)
        return copies

    def gather_start(copies):
        for q in range(4):
            copies['x', q].start()
            copies['y', q].start()
            if q == 0:
                copies['own'].start()

    def gather_need(copies, c):
        if c == 2:
            copies['own'].wait_recv()
        if 4 <= c < 12:
            q = (c - 4) // 2
            if c % 2 == 0:
                copies['both', q].wait_recv()
                copies['across', q].start()
                copies['x core', q].start()
                copies['y core', q].start()
            else:
                copies['both core', q].wait_recv()
        if c >= 12:
            h = (c - 12) // 2
            if c % 2 == 0:
                copies['across both', h].wait_recv()
                copies['across core', h].start()
            else:
                copies['across core', h].wait_recv()

    def mask_value(k):
        return block_mask[me, partner(k)].astype(F32)

    def forward_pass(copies, y, first, segments):
        width = y.shape[1]
        for begin, per_step, steps in segments:
            def step(i, carry, begin=begin, per_step=per_step, steps=steps):
                for at in range(steps):
                    needs = [begin + at * per_step + j for j in range(per_step)]
                    if any(c == 2 or c >= 4 for c in needs):
                        @pl.when(i == at)
                        def _(needs=needs):
                            for c in needs:
                                gather_need(copies, c)
                total = None
                for j in range(per_step):
                    c = begin + i * per_step + j
                    for part in range(2):
                        k, q = block_quart(c, part)
                        cols = pl.ds(pl.multiple_of(q * QUART, QUART), QUART)
                        ymask[:width, (2 * j + part) * QUART:(2 * j + part + 1) * QUART] = (y[k, :, cols].astype(F32) * mask_value(k)).astype(BF16)
                for j in range(per_step):
                    fetch(first + begin + i * per_step + j).wait()
                for j in range(per_step):
                    fetch(first + begin + i * per_step + j + SLOTS - 2).start()
                for j in range(per_step):
                    g = first + begin + i * per_step + j
                    term = lax.dot_general(abuf[lax.rem(g, SLOTS)], ymask[:width, j * HALF:(j + 1) * HALF], NT, preferred_element_type=F32)
                    total = term if total is None else total + term
                acc[:, :width] += total
                return carry
            lax.fori_loop(0, steps, step, 0)

    copies1 = gather_copies(yall, 0, 0)
    gather_start(copies1)
    acc[...] = jnp.zeros_like(acc)
    forward_pass(copies1, yall, 0, ((0, 2, 2), (4, 1, 1), (5, 2, 3), (11, 1, 5)))

    hid[...] = jnp.maximum(acc[...], 0.0).astype(BF16)
    y2all[0] = lax.dot_general(wot_bf, hid[...], NT, preferred_element_type=F32).astype(BF16)

    copies2 = gather_copies(y2all, 1, 13)
    gather_start(copies2)
    count_copies = [remote(cnt.at[0], cnt.at[k], k, 2, 26) for k in range(1, DEVICES)]
    counts = remote(cnt.at[pl.ds(1, 7)], cnt.at[pl.ds(1, 7)], 1, 2, 26)
    for copy in count_copies:
        copy.start()
    copies1['sent'].wait_send()
    ident = (lax.broadcasted_iota(jnp.int32, (HID, HID), 0) == lax.broadcasted_iota(jnp.int32, (HID, HID), 1)).astype(BF16)
    hidt[...] = lax.dot_general(ident, hid[...], NT, preferred_element_type=F32).astype(BF16)
    acc[...] = jnp.zeros_like(acc)

    forward_pass(copies2, y2all, CHUNKS, ((0, 2, 2), (4, 1, 1), (5, 2, 5), (15, 1, 1)))

    for i in range(ROWS // 128):
        at = pl.ds(i * 128, 128)
        pb[0, :C_PAD, at] = acc[at, :].T[:C_PAD]
    counts.wait_recv()
    label_count = cnt[0, 0:1, 0:1]
    for k in range(1, DEVICES):
        label_count = label_count + cnt[k, 0:1, 0:1]
    loss = jnp.zeros((1, 1), F32)
    lhs[C_PAD:, :] = jnp.zeros((HID - C_PAD, ROWS), BF16)
    for q in range(4):
        at = pl.ds(q * QUART, QUART)
        z = pb[0, :C_PAD, at]
        row = lax.broadcasted_iota(jnp.int32, (C_PAD, QUART), 0)
        z = jnp.where(row < CLASSES, z, -jnp.inf)
        top = jnp.max(z, axis=0, keepdims=True)
        log_norm = jnp.log(jnp.sum(jnp.exp(z - top), axis=0, keepdims=True)) + top
        hot = row == labels[:, at]
        picked = jnp.sum(jnp.where(hot, z, 0.0), axis=0, keepdims=True)
        w = mask[:, at].astype(F32)
        loss = loss + jnp.sum(w * (log_norm - picked), axis=1, keepdims=True)
        prob = jnp.exp(z - log_norm)
        lhs[:C_PAD, at] = ((prob - hot.astype(F32)) * (w / label_count)).astype(BF16)

    def scatter_copies(p, r, f, ix, send, recv):
        def half(k, h):
            return p.at[k, :, pl.ds(h * HALF, HALF)]

        def quart(k, q):
            return p.at[k, :, pl.ds(q * QUART, QUART)]

        copies = {'sent': remote(p.at[pl.ds(0, 7)], p.at[pl.ds(0, 7)], 1, send, recv)}
        for h in range(2):
            even, odd = 2 * h, 2 * h + 1
            for k in (7, 5, 3, 1):
                copies['core', k, h] = remote(half(k, h), r.at[k // 2, h], 1, send, recv + k - 1 + h)
            copies['xy', h] = remote(quart(6, even), f.at[0, h], 2, send, recv + 8 + h)
            copies['yx', h] = remote(quart(6, odd), f.at[1, h], 4, send, recv + 10 + h)
            copies['y raw', h] = remote(quart(4, odd), ix.at[1, odd], 4, send, recv + 12 + odd)
            copies['x raw', h] = remote(quart(2, even), ix.at[0, even], 2, send, recv + 12 + even)
            copies['y', h] = remote(quart(4, even), ix.at[1, even], 4, send, recv + 12 + even)
            copies['x', h] = remote(quart(2, odd), ix.at[0, odd], 2, send, recv + 12 + odd)
            copies['both', even] = remote(half(0, 0), half(0, 0), 2, send, recv + 12 + even)
            copies['both', odd] = remote(half(0, 0), half(0, 0), 2, send, recv + 12 + odd)
        return copies

    def scatter_events(copies, p, r, f, c, pass_on):
        sends = {6: ('xy', 'yx'), 4: ('y raw',), 2: ('x raw',), 0: ()}
        order = [(7, 0), (6, 0), (7, 1), (6, 1)] + [(k, h) for h in range(2) for k in (5, 4, 3, 2)] + [(1, 0), (0, 0), (1, 1), (0, 1)]
        for at, (k, h) in enumerate(order):
            @pl.when(c == at)
            def _(at=at, k=k, h=h):
                if k % 2 == 1:
                    copies['core', k, h].start()
                else:
                    cols = pl.ds(h * HALF, HALF)
                    copies['core', k + 1, h].wait_recv()
                    p[k, :, cols] = p[k, :, cols] + r[k // 2, h]
                    for name in sends[k]:
                        copies[name, h].start()
                for way, h2 in pass_on.get(at, ()):
                    if way == 'y':
                        even = pl.ds(2 * h2 * QUART, QUART)
                        copies['xy', h2].wait_recv()
                        p[4, :, even] = p[4, :, even] + f[0, h2]
                    else:
                        odd = pl.ds((2 * h2 + 1) * QUART, QUART)
                        copies['yx', h2].wait_recv()
                        p[2, :, odd] = p[2, :, odd] + f[1, h2]
                    copies[way, h2].start()

    def scatter_result(copies, p, ix, q):
        copies['both', q].wait_recv()
        return (p[0, :, pl.ds(q * QUART, QUART)] + ix[0, q] + ix[1, q]).astype(BF16)

    pa = pb.at[:, pl.ds(0, C_PAD), :]
    copies3 = scatter_copies(pa, ra, fa, ia, 3, 27)

    def pass3(c, carry):
        g = c + 2 * CHUNKS
        k, q = block_quart(g, 0)
        cols = pl.ds(pl.multiple_of(q * QUART, HALF), HALF)
        fetch(g).wait()
        fetch(g + SLOTS - 2).start()
        part = jnp.dot(lhs[...], abuf[lax.rem(g, SLOTS)], preferred_element_type=F32)
        pa[k, :, cols] = part[:C_PAD] * mask_value(k)
        scatter_events(copies3, pa, ra, fa, c, {6: (('y', 0),), 7: (('x', 0),), 9: (('y', 1),), 11: (('x', 1),)})
        return carry
    lax.fori_loop(0, CHUNKS, pass3, 0)
    d2t = jnp.concatenate([scatter_result(copies3, pa, ia, q) for q in range(4)], axis=1)
    back = jnp.dot(wo_bf, d2t, preferred_element_type=F32)
    lhs[...] = jnp.where(hidt[...].astype(F32) > 0.0, back, 0.0).astype(BF16)

    copies3['sent'].wait_send()

    copies4 = scatter_copies(pb, rb, fb, ib, 4, 43)

    def pass4(c, carry):
        g = c + 3 * CHUNKS
        k, q = block_quart(g, 0)
        cols = pl.ds(pl.multiple_of(q * QUART, HALF), HALF)
        fetch(g).wait()

        @pl.when(g + SLOTS - 2 < 4 * CHUNKS)
        def _():
            fetch(g + SLOTS - 2).start()
        part = jnp.dot(lhs[...], abuf[lax.rem(g, SLOTS)], preferred_element_type=F32)
        pb[k, :, cols] = part * mask_value(k)
        scatter_events(copies4, pb, rb, fb, c, {9: (('y', 0),), 10: (('x', 0),), 13: (('y', 1), ('x', 1))})
        return carry
    lax.fori_loop(0, CHUNKS, pass4, 0)

    gpart[F_IN // 8 * 8:GWO_ROW, :] = jnp.zeros((8, HID), F32)
    gpart[GWO_ROW:LOSS_ROW, :] = jnp.dot(d2t, hid[...], preferred_element_type=F32)
    gpart[LOSS_ROW:SUM_ROWS, :] = jnp.broadcast_to(loss / label_count, (SUM_ROWS - LOSS_ROW, HID))
    copies2['sent'].wait_send()
    counts.wait_send()
    for q in range(4):
        term = lax.dot_general(xbuf[:, q * QUART:(q + 1) * QUART], scatter_result(copies4, pb, ib, q), NT, preferred_element_type=F32)
        if q == 0:
            gpart[:F_IN, :] = term
        else:
            gpart[:F_IN, :] += term

    half_rows, quart_rows = SUM_ROWS // 2, SUM_ROWS // 4
    mine = pl.ds(pl.multiple_of(bits[0] * half_rows, 8), half_rows)
    other = pl.ds(pl.multiple_of((1 - bits[0]) * half_rows, 8), half_rows)
    swap = remote(gpart.at[other, :], gpair, 1, 5, 59)
    swap.start()
    swap.wait()
    gpart[mine, :] = gpart[mine, :] + gpair[...]
    first = [{}, {}]
    pieces = [(q, begin, size) for begin, size in ((0, 88), (88, quart_rows - 88)) for q in range(2)]
    rows = []
    for n, (q, begin, size) in enumerate(pieces):
        at = pl.ds(pl.multiple_of(bits[0] * half_rows + q * quart_rows + begin, 8), size)
        rows.append(at)
        for step in range(2):
            way = (2, 4)[(q + step) % 2]
            first[step][n] = remote(gpart.at[at, :], gacross.at[step, q, pl.ds(begin, size), :], way, 6 + 4 * step + n, 60 + 4 * step + n)
        first[0][n].start()
    for step in range(2):
        for n, (q, begin, size) in enumerate(pieces):
            first[step][n].wait()
            gpart[rows[n], :] = gpart[rows[n], :] + gacross[step, q, begin:begin + size, :]
            if step == 0:
                first[1][n].start()
    final = remote(gpart.at[mine, :], sums_out.at[mine, :], 1, 14, 68)
    final.start()
    keep = pltpu.make_async_copy(gpart.at[mine, :], sums_out.at[mine, :], xsem.at[0])
    keep.start()
    copies4['sent'].wait_send()
    keep.wait()
    final.wait()


def cut_kernel(sums, loss_out, gwh_out, gwo_out):
    gwh_out[...] = sums[:F_IN, :]
    gwo_out[...] = sums[GWO_ROW:GWO_ROW + CLASSES, :]
    loss_out[...] = sums[LOSS_ROW:LOSS_ROW + 1, 0:1]


def device_step(adj, feat, w_hidden, w_output, labels, train_mask, block_mask):
    vmem = pl.BlockSpec(memory_space=pltpu.VMEM)
    hbm = pl.BlockSpec(memory_space=pl.ANY)
    v = pltpu.VMEM
    sends, arrivals = 15, 69
    sums = pl.pallas_call(
        step_kernel,
        out_shape=jax.ShapeDtypeStruct((SUM_ROWS, HID), F32),
        in_specs=[hbm] * 6 + [pl.BlockSpec(memory_space=pltpu.SMEM)],
        out_specs=hbm,
        scratch_shapes=[
            v((SLOTS, ROWS, HALF), BF16), v((F_IN, ROWS), BF16), v((F_IN, HID), F32), v((CLASSES, HID), F32), v((1, ROWS), jnp.int32), v((1, ROWS), jnp.int32), v((ROWS, HID), F32),
            v((DEVICES, HID, ROWS), BF16), v((DEVICES, C_PAD, ROWS), BF16), v((HID, ROWS), BF16), v((ROWS, HID), BF16),
            v((HID, ROWS), BF16), v((128, 128), F32), v((HID, ROWS), BF16),
            v((DEVICES, 8, 128), F32),
            v((4, 2, C_PAD, HALF), F32), v((2, 2, C_PAD, QUART), F32), v((2, 4, C_PAD, QUART), F32),
            v((DEVICES, HID, ROWS), F32), v((4, 2, HID, HALF), F32), v((2, 2, HID, QUART), F32), v((2, 4, HID, QUART), F32),
            v((SUM_ROWS, HID), F32), v((SUM_ROWS // 2, HID), F32), v((2, 2, SUM_ROWS // 4, HID), F32),
            pltpu.SemaphoreType.DMA((SLOTS, 2)), pltpu.SemaphoreType.DMA((5,)),
            pltpu.SemaphoreType.DMA((sends,)), pltpu.SemaphoreType.DMA((arrivals,)),
        ],
        compiler_params=pltpu.CompilerParams(collective_id=0, has_side_effects=True, vmem_limit_bytes=67043328),
        name='gcn_step',
    )(adj, feat.T, w_hidden, w_output.T, labels.reshape(1, ROWS), train_mask.reshape(1, ROWS), block_mask)
    loss, gwh, gwo = pl.pallas_call(
        cut_kernel,
        out_shape=(jax.ShapeDtypeStruct((1, 1), F32), jax.ShapeDtypeStruct((F_IN, HID), F32), jax.ShapeDtypeStruct((CLASSES, HID), F32)),
        in_specs=[vmem],
        out_specs=(vmem, vmem, vmem),
        compiler_params=pltpu.CompilerParams(vmem_limit_bytes=4 * 2**20),
        name='cut',
    )(sums)
    return loss[0, 0], gwh, gwo.T


def solution(mesh):
    row_spec = P(AXIS_NAME, None)
    vec_spec = P(AXIS_NAME)
    return jax.shard_map(device_step, mesh=mesh, in_specs=(row_spec, row_spec, P(), P(), vec_spec, vec_spec, P()), out_specs=(P(), P(), P()), check_vma=False)
```

```python
import jax
import jax.numpy as jnp
from jax import lax
from jax.experimental import pallas as pl
from jax.experimental.pallas import tpu as pltpu
from jax.sharding import PartitionSpec as P

AXIS_NAME = 'nodes'
MESH = pl.DeviceIdType.MESH
F32, BF16 = jnp.float32, jnp.bfloat16
DEVICES = 8
ROWS = 2048
NODES = DEVICES * ROWS
F_IN = 602
HID = 128
CLASSES = 41
C_PAD = 48
HALF = ROWS // 2
QUART = ROWS // 4
SLOTS = 7
CHUNKS = NODES // HALF
SUM_ROWS = 672
GWO_ROW = 608
LOSS_ROW = GWO_ROW + C_PAD
NT = (((1,), (1,)), ((), ()))


def step_kernel(adj, feat, wh_in, wo_in, labels_in, mask_in, block_mask, sums_out,
                abuf, xbuf, wh, wo, labels, mask, acc, yall, y2all, ymask, hid, hidt, wpad, lhs, cnt,
                ra, fa, ia, pb, rb, fb, ib, gpart, gpair, gacross,
                asem, xsem, ssem, rsem):
    me = lax.axis_index(AXIS_NAME)
    bits = (lax.rem(me, 2), lax.rem(me // 2, 2), me // 4)

    def partner(k):
        return lax.rem(bits[0] + k, 2) + 2 * lax.rem(bits[1] + k // 2, 2) + 4 * lax.rem(bits[2] + k // 4, 2)

    peers = [partner(k) for k in range(DEVICES)]

    def block_quart(g, i):
        back = lax.div(g, 2 * CHUNKS)
        c = lax.rem(g, CHUNKS)
        q, r = lax.div(c, 4), lax.rem(c, 4)
        mid = lax.div(q * (3 - q), 2)
        last = lax.div(q, 3)
        pair, odd = lax.div(c, 2), lax.rem(c, 2)
        forth_k = mid * (2 + odd + 2 * i) + (1 - mid) * (last * (6 + odd) + (1 - last) * pair)
        forth_q = mid * (pair - 2) + (1 - mid) * (2 * (last * (pair - 6) + (1 - last) * odd) + i)
        back_k, back_h = mid * (5 - r) + (1 - mid) * (7 - 6 * last - odd), mid * (q - 1) + (1 - mid) * lax.div(r, 2)
        return back * back_k + (1 - back) * forth_k, back * (2 * back_h + i) + (1 - back) * forth_q

    class Fetch:
        def __init__(self, g):
            slot = lax.rem(g, SLOTS)
            self.pieces = []
            for i in range(2):
                k, q = block_quart(g, i)
                col = pl.multiple_of(partner(k) * ROWS + q * QUART, QUART)
                self.pieces.append(pltpu.make_async_copy(adj.at[:, pl.ds(col, QUART)], abuf.at[slot, :, pl.ds(i * QUART, QUART)], asem.at[slot]))
            self.whole = pltpu.make_async_copy(adj.at[:, pl.ds(0, HALF)], abuf.at[slot], asem.at[slot])

        def start(self):
            for piece in self.pieces:
                piece.start()

        def wait(self):
            self.whole.wait()

    fetch = Fetch

    def remote(src, dst, k, send, recv):
        return pltpu.make_async_remote_copy(src_ref=src, dst_ref=dst, send_sem=ssem.at[send], recv_sem=rsem.at[recv],
                                            device_id=(peers[k],), device_id_type=MESH)

    xcopy = pltpu.make_async_copy(feat, xbuf, xsem.at[0])
    whcopy = pltpu.make_async_copy(wh_in, wh, xsem.at[1])
    whcopy.start()
    xcopy.start()
    small = [pltpu.make_async_copy(src, dst, xsem.at[2 + i]) for i, (src, dst) in
             enumerate(((wo_in, wo), (labels_in, labels), (mask_in, mask)))]
    for copy in small:
        copy.start()
    barrier = pltpu.get_barrier_semaphore()
    for k in range(1, DEVICES):
        pl.semaphore_signal(barrier, inc=1, device_id=(peers[k],), device_id_type=MESH)
    whcopy.wait()
    wh_t = wh[...].T.astype(BF16)
    xcopy.wait()
    for g in range(SLOTS - 2):
        fetch(jnp.int32(g)).start()

    def gather_copies(y, send, recv):
        def half(k, h):
            return y.at[k, :, pl.ds(h * HALF, HALF)]

        def quart(k, q):
            return y.at[k, :, pl.ds(q * QUART, QUART)]

        copies = {'own': remote(y.at[0], y.at[1], 1, send, recv)}
        for q in range(4):
            copies['x', q] = remote(quart(0, q), quart(2, q), 2, send, recv + 1 + q)
            copies['y', q] = remote(quart(0, q), quart(4, q), 4, send, recv + 1 + q)
            copies['x core', q] = remote(quart(2, q), quart(3, q), 1, send, recv + 5 + q)
            copies['y core', q] = remote(quart(4, q), quart(5, q), 1, send, recv + 5 + q)
            copies['both', q] = remote(half(0, 0), half(0, 0), 2, send, recv + 1 + q)
            copies['both core', q] = remote(half(0, 0), half(0, 0), 1, send, recv + 5 + q)
            if q % 2 == 0:
                copies['across', q] = remote(quart(2, q), quart(6, q), 4, send, recv + 9 + q // 2)
            else:
                copies['across', q] = remote(quart(4, q), quart(6, q), 2, send, recv + 9 + q // 2)
        for h in range(2):
            copies['across both', h] = remote(half(0, 0), half(0, 0), 2, send, recv + 9 + h)
            copies['across core', h] = remote(half(6, h), half(7, h), 1, send, recv + 11 + h)
        copies['sent'] = remote(y.at[pl.ds(0, 7)], y.at[pl.ds(0, 7)], 1, send, recv)
        return copies

    def gather_start(copies, quarters=range(4)):
        for q in quarters:
            copies['x', q].start()
            copies['y', q].start()
            if q == 3:
                copies['own'].start()

    def gather_need(copies, c):
        if c == 2:
            copies['own'].wait_recv()
        if 4 <= c < 12:
            q = (c - 4) // 2
            if c % 2 == 0:
                copies['both', q].wait_recv()
                copies['across', q].start()
                copies['x core', q].start()
                copies['y core', q].start()
            else:
                copies['both core', q].wait_recv()
        if c >= 12:
            h = (c - 12) // 2
            if c % 2 == 0:
                copies['across both', h].wait_recv()
                copies['across core', h].start()
            else:
                copies['across core', h].wait_recv()

    def mask_value(k):
        return block_mask[me, partner(k)].astype(F32)

    def forward_pass(copies, y, first, segments):
        width = y.shape[1]
        for begin, per_step, steps in segments:
            def step(i, carry, begin=begin, per_step=per_step, steps=steps):
                for at in range(steps):
                    needs = [begin + at * per_step + j for j in range(per_step)]
                    if any(c == 2 or c >= 4 for c in needs):
                        @pl.when(i == at)
                        def _(needs=needs):
                            for c in needs:
                                gather_need(copies, c)
                total = None
                for j in range(per_step):
                    c = begin + i * per_step + j
                    for part in range(2):
                        k, q = block_quart(c, part)
                        cols = pl.ds(pl.multiple_of(q * QUART, QUART), QUART)
                        ymask[:width, (2 * j + part) * QUART:(2 * j + part + 1) * QUART] = (y[k, :, cols].astype(F32) * mask_value(k)).astype(BF16)
                for j in range(per_step):
                    fetch(first + begin + i * per_step + j).wait()
                for j in range(per_step):
                    fetch(first + begin + i * per_step + j + SLOTS - 2).start()
                for j in range(per_step):
                    g = first + begin + i * per_step + j
                    term = lax.dot_general(abuf[lax.rem(g, SLOTS)], ymask[:width, j * HALF:(j + 1) * HALF], NT, preferred_element_type=F32)
                    total = term if total is None else total + term
                acc[:, :width] += total
                return carry
            lax.fori_loop(0, steps, step, 0)

    copies1 = gather_copies(yall, 0, 0)
    for h in range(2):
        at = pl.ds(h * HALF, HALF)
        yall[0, :, at] = jnp.dot(wh_t, xbuf[:, at], preferred_element_type=F32).astype(BF16)
        if h == 0:
            pl.semaphore_wait(barrier, DEVICES - 1)
        gather_start(copies1, (2 * h, 2 * h + 1))
    acc[...] = jnp.zeros_like(acc)
    for copy in small:
        copy.wait()
    wpad[...] = jnp.zeros_like(wpad)
    wpad[:CLASSES, :] = wo[...]
    wot_bf = wpad[:C_PAD, :].astype(BF16)
    wo_bf = wpad[...].T[:, :C_PAD].astype(BF16)
    cnt[0] = jnp.broadcast_to(jnp.sum(mask[...].astype(F32), axis=1, keepdims=True), (8, 128))
    forward_pass(copies1, yall, 0, ((0, 2, 2), (4, 1, 12)))

    hid[...] = jnp.maximum(acc[...], 0.0).astype(BF16)
    y2all[0] = lax.dot_general(wot_bf, hid[...], NT, preferred_element_type=F32).astype(BF16)

    copies2 = gather_copies(y2all, 1, 13)
    gather_start(copies2)
    count_copies = [remote(cnt.at[0], cnt.at[k], k, 2, 26) for k in range(1, DEVICES)]
    counts = remote(cnt.at[pl.ds(1, 7)], cnt.at[pl.ds(1, 7)], 1, 2, 26)
    for copy in count_copies:
        copy.start()
    copies1['sent'].wait_send()
    ident = (lax.broadcasted_iota(jnp.int32, (HID, HID), 0) == lax.broadcasted_iota(jnp.int32, (HID, HID), 1)).astype(BF16)
    hidt[...] = lax.dot_general(ident, hid[...], NT, preferred_element_type=F32).astype(BF16)
    acc[...] = jnp.zeros_like(acc)

    forward_pass(copies2, y2all, CHUNKS, ((0, 2, 2), (4, 1, 1), (5, 2, 5), (15, 1, 1)))

    for i in range(ROWS // 128):
        at = pl.ds(i * 128, 128)
        pb[0, :C_PAD, at] = acc[at, :].T[:C_PAD]
    counts.wait_recv()
    label_count = cnt[0, 0:1, 0:1]
    for k in range(1, DEVICES):
        label_count = label_count + cnt[k, 0:1, 0:1]
    loss = jnp.zeros((1, 1), F32)
    lhs[C_PAD:, :] = jnp.zeros((HID - C_PAD, ROWS), BF16)
    for q in range(4):
        at = pl.ds(q * QUART, QUART)
        z = pb[0, :C_PAD, at]
        row = lax.broadcasted_iota(jnp.int32, (C_PAD, QUART), 0)
        z = jnp.where(row < CLASSES, z, -jnp.inf)
        top = jnp.max(z, axis=0, keepdims=True)
        log_norm = jnp.log(jnp.sum(jnp.exp(z - top), axis=0, keepdims=True)) + top
        hot = row == labels[:, at]
        picked = jnp.sum(jnp.where(hot, z, 0.0), axis=0, keepdims=True)
        w = mask[:, at].astype(F32)
        loss = loss + jnp.sum(w * (log_norm - picked), axis=1, keepdims=True)
        prob = jnp.exp(z - log_norm)
        lhs[:C_PAD, at] = ((prob - hot.astype(F32)) * (w / label_count)).astype(BF16)

    def scatter_copies(p, r, f, ix, send, recv):
        def half(k, h):
            return p.at[k, :, pl.ds(h * HALF, HALF)]

        def quart(k, q):
            return p.at[k, :, pl.ds(q * QUART, QUART)]

        copies = {'sent': remote(p.at[pl.ds(0, 7)], p.at[pl.ds(0, 7)], 1, send, recv)}
        for h in range(2):
            even, odd = 2 * h, 2 * h + 1
            for k in (7, 5, 3, 1):
                copies['core', k, h] = remote(half(k, h), r.at[k // 2, h], 1, send, recv + k - 1 + h)
            copies['xy', h] = remote(quart(6, even), f.at[0, h], 2, send, recv + 8 + h)
            copies['yx', h] = remote(quart(6, odd), f.at[1, h], 4, send, recv + 10 + h)
            copies['y raw', h] = remote(quart(4, odd), ix.at[1, odd], 4, send, recv + 12 + odd)
            copies['x raw', h] = remote(quart(2, even), ix.at[0, even], 2, send, recv + 12 + even)
            copies['y', h] = remote(quart(4, even), ix.at[1, even], 4, send, recv + 12 + even)
            copies['x', h] = remote(quart(2, odd), ix.at[0, odd], 2, send, recv + 12 + odd)
            copies['both', even] = remote(half(0, 0), half(0, 0), 2, send, recv + 12 + even)
            copies['both', odd] = remote(half(0, 0), half(0, 0), 2, send, recv + 12 + odd)
        return copies

    def scatter_events(copies, p, r, f, c, pass_on):
        sends = {6: ('xy', 'yx'), 4: ('y raw',), 2: ('x raw',), 0: ()}
        order = [(7, 0), (6, 0), (7, 1), (6, 1)] + [(k, h) for h in range(2) for k in (5, 4, 3, 2)] + [(1, 0), (0, 0), (1, 1), (0, 1)]
        for at, (k, h) in enumerate(order):
            @pl.when(c == at)
            def _(at=at, k=k, h=h):
                if k % 2 == 1:
                    copies['core', k, h].start()
                else:
                    cols = pl.ds(h * HALF, HALF)
                    copies['core', k + 1, h].wait_recv()
                    p[k, :, cols] = p[k, :, cols] + r[k // 2, h]
                    for name in sends[k]:
                        copies[name, h].start()
                for way, h2 in pass_on.get(at, ()):
                    if way == 'y':
                        even = pl.ds(2 * h2 * QUART, QUART)
                        copies['xy', h2].wait_recv()
                        p[4, :, even] = p[4, :, even] + f[0, h2]
                    else:
                        odd = pl.ds((2 * h2 + 1) * QUART, QUART)
                        copies['yx', h2].wait_recv()
                        p[2, :, odd] = p[2, :, odd] + f[1, h2]
                    copies[way, h2].start()

    def scatter_result(copies, p, ix, q):
        copies['both', q].wait_recv()
        return (p[0, :, pl.ds(q * QUART, QUART)] + ix[0, q] + ix[1, q]).astype(BF16)

    pa = pb.at[:, pl.ds(0, C_PAD), :]
    copies3 = scatter_copies(pa, ra, fa, ia, 3, 27)

    def pass3(c, carry):
        g = c + 2 * CHUNKS
        k, q = block_quart(g, 0)
        cols = pl.ds(pl.multiple_of(q * QUART, HALF), HALF)
        fetch(g).wait()
        fetch(g + SLOTS - 2).start()
        part = jnp.dot(lhs[...], abuf[lax.rem(g, SLOTS)], preferred_element_type=F32)
        pa[k, :, cols] = part[:C_PAD] * mask_value(k)
        scatter_events(copies3, pa, ra, fa, c, {6: (('y', 0),), 7: (('x', 0),), 9: (('y', 1),), 11: (('x', 1),)})
        return carry
    lax.fori_loop(0, CHUNKS, pass3, 0)
    copies2['sent'].wait_send()
    d2t = y2all.at[0]
    for q in range(4):
        at = pl.ds(q * QUART, QUART)
        d2t[:, at] = scatter_result(copies3, pa, ia, q)
        back = jnp.dot(wo_bf, d2t[:, at], preferred_element_type=F32)
        lhs[:, at] = jnp.where(hidt[:, at].astype(F32) > 0.0, back, 0.0).astype(BF16)
    copies3['sent'].wait_send()

    copies4 = scatter_copies(pb, rb, fb, ib, 4, 43)

    def pass4(c, carry):
        g = c + 3 * CHUNKS
        k, q = block_quart(g, 0)
        cols = pl.ds(pl.multiple_of(q * QUART, HALF), HALF)
        fetch(g).wait()

        @pl.when(g + SLOTS - 2 < 4 * CHUNKS)
        def _():
            fetch(g + SLOTS - 2).start()
        part = jnp.dot(lhs[...], abuf[lax.rem(g, SLOTS)], preferred_element_type=F32)
        pb[k, :, cols] = part * mask_value(k)
        scatter_events(copies4, pb, rb, fb, c, {9: (('y', 0),), 10: (('x', 0),), 13: (('y', 1), ('x', 1))})
        return carry
    lax.fori_loop(0, CHUNKS, pass4, 0)

    gpart[F_IN // 8 * 8:GWO_ROW, :] = jnp.zeros((8, HID), F32)
    gpart[GWO_ROW:LOSS_ROW, :] = jnp.dot(d2t[...], hid[...], preferred_element_type=F32)
    gpart[LOSS_ROW:SUM_ROWS, :] = jnp.broadcast_to(loss / label_count, (SUM_ROWS - LOSS_ROW, HID))
    counts.wait_send()
    for h in range(2):
        d1t = jnp.concatenate([scatter_result(copies4, pb, ib, 2 * h + q) for q in range(2)], axis=1)
        term = lax.dot_general(xbuf[:, h * HALF:(h + 1) * HALF], d1t, NT, preferred_element_type=F32)
        if h == 0:
            gpart[:F_IN, :] = term
        else:
            gpart[:F_IN, :] += term

    half_rows, quart_rows = SUM_ROWS // 2, SUM_ROWS // 4
    mine = pl.ds(pl.multiple_of(bits[0] * half_rows, 8), half_rows)
    other = pl.ds(pl.multiple_of((1 - bits[0]) * half_rows, 8), half_rows)
    swap = remote(gpart.at[other, :], gpair, 1, 5, 59)
    swap.start()
    swap.wait()
    gpart[mine, :] = gpart[mine, :] + gpair[...]
    first = [{}, {}]
    pieces = [(q, begin, size) for begin, size in ((0, 88), (88, quart_rows - 88)) for q in range(2)]
    rows = []
    for n, (q, begin, size) in enumerate(pieces):
        at = pl.ds(pl.multiple_of(bits[0] * half_rows + q * quart_rows + begin, 8), size)
        rows.append(at)
        for step in range(2):
            way = (2, 4)[(q + step) % 2]
            first[step][n] = remote(gpart.at[at, :], gacross.at[step, q, pl.ds(begin, size), :], way, 6 + 4 * step + n, 60 + 4 * step + n)
        first[0][n].start()
    for step in range(2):
        for n, (q, begin, size) in enumerate(pieces):
            first[step][n].wait()
            gpart[rows[n], :] = gpart[rows[n], :] + gacross[step, q, begin:begin + size, :]
            if step == 0:
                first[1][n].start()
    final = remote(gpart.at[mine, :], sums_out.at[mine, :], 1, 14, 68)
    final.start()
    sums_out[mine, :] = gpart[mine, :]
    copies4['sent'].wait_send()
    final.wait()


def cut_kernel(sums, loss_out, gwh_out, gwo_out):
    gwh_out[...] = sums[:F_IN, :]
    gwo_out[...] = sums[GWO_ROW:GWO_ROW + CLASSES, :]
    loss_out[...] = sums[LOSS_ROW:LOSS_ROW + 1, 0:1]


def device_step(adj, feat, w_hidden, w_output, labels, train_mask, block_mask):
    vmem = pl.BlockSpec(memory_space=pltpu.VMEM)
    hbm = pl.BlockSpec(memory_space=pl.ANY)
    v = pltpu.VMEM
    sends, arrivals = 15, 69
    sums = pl.pallas_call(
        step_kernel,
        out_shape=pltpu.VMEM((SUM_ROWS, HID), F32),
        in_specs=[hbm] * 6 + [pl.BlockSpec(memory_space=pltpu.SMEM)],
        out_specs=vmem,
        scratch_shapes=[
            v((SLOTS, ROWS, HALF), BF16), v((F_IN, ROWS), BF16), v((F_IN, HID), F32), v((CLASSES, HID), F32), v((1, ROWS), jnp.int32), v((1, ROWS), jnp.int32), v((ROWS, HID), F32),
            v((DEVICES, HID, ROWS), BF16), v((DEVICES, C_PAD, ROWS), BF16), v((HID, ROWS), BF16), v((ROWS, HID), BF16),
            v((HID, ROWS), BF16), v((128, 128), F32), v((HID, ROWS), BF16),
            v((DEVICES, 8, 128), F32),
            v((4, 2, C_PAD, HALF), F32), v((2, 2, C_PAD, QUART), F32), v((2, 4, C_PAD, QUART), F32),
            v((DEVICES, HID, ROWS), F32), v((4, 2, HID, HALF), F32), v((2, 2, HID, QUART), F32), v((2, 4, HID, QUART), F32),
            v((SUM_ROWS, HID), F32), v((SUM_ROWS // 2, HID), F32), v((2, 2, SUM_ROWS // 4, HID), F32),
            pltpu.SemaphoreType.DMA((SLOTS,)), pltpu.SemaphoreType.DMA((5,)),
            pltpu.SemaphoreType.DMA((sends,)), pltpu.SemaphoreType.DMA((arrivals,)),
        ],
        compiler_params=pltpu.CompilerParams(collective_id=0, has_side_effects=True, vmem_limit_bytes=62 * 2**20),
        name='gcn_step',
    )(adj, feat.T, w_hidden, w_output.T, labels.reshape(1, ROWS), train_mask.reshape(1, ROWS), block_mask)
    loss, gwh, gwo = pl.pallas_call(
        cut_kernel,
        out_shape=(jax.ShapeDtypeStruct((1, 1), F32), jax.ShapeDtypeStruct((F_IN, HID), F32), jax.ShapeDtypeStruct((CLASSES, HID), F32)),
        in_specs=[vmem],
        out_specs=(vmem, vmem, vmem),
        compiler_params=pltpu.CompilerParams(vmem_limit_bytes=4 * 2**20),
        name='cut',
    )(sums)
    return loss[0, 0], gwh, gwo.T


def solution(mesh):
    row_spec = P(AXIS_NAME, None)
    vec_spec = P(AXIS_NAME)
    return jax.shard_map(device_step, mesh=mesh, in_specs=(row_spec, row_spec, P(), P(), vec_spec, vec_spec, P()), out_specs=(P(), P(), P()), check_vma=False)
```

```python
import jax
import jax.numpy as jnp
from jax import lax
from jax.experimental import pallas as pl
from jax.experimental.pallas import tpu as pltpu
from jax.sharding import PartitionSpec as P

AXIS_NAME = 'nodes'
MESH = pl.DeviceIdType.MESH
F32, BF16 = jnp.float32, jnp.bfloat16
DEVICES = 8
ROWS = 2048
NODES = DEVICES * ROWS
F_IN = 602
HID = 128
CLASSES = 41
C_PAD = 48
HALF = ROWS // 2
QUART = ROWS // 4
SLOTS = 7
CHUNKS = NODES // HALF
SUM_ROWS = 672
GWO_ROW = 608
LOSS_ROW = GWO_ROW + C_PAD
NT = (((1,), (1,)), ((), ()))


def div(a, b):
    return a // b if isinstance(a, int) else lax.div(a, b)


def rem(a, b):
    return a % b if isinstance(a, int) else lax.rem(a, b)


def step_kernel(adj, feat, wh_in, wo_in, labels_in, mask_in, block_mask, sums_out,
                abuf, xbuf, wh, wo, labels, mask, acc, yall, y2all, ymask, hid, hidt, wpad, lhs, cnt,
                ra, fa, ia, pb, rb, fb, ib, gpart, gpair, gacross,
                asem, xsem, ssem, rsem):
    me = lax.axis_index(AXIS_NAME)
    bits = (lax.rem(me, 2), lax.rem(me // 2, 2), me // 4)

    def partner(k):
        return lax.rem(bits[0] + k, 2) + 2 * lax.rem(bits[1] + div(k, 2), 2) + 4 * lax.rem(bits[2] + div(k, 4), 2)

    peers = [partner(k) for k in range(DEVICES)]

    def block_quart(g, i):
        back = div(g, 2 * CHUNKS)
        c = rem(g, CHUNKS)
        q, r = div(c, 4), rem(c, 4)
        mid = div(q * (3 - q), 2)
        last = div(q, 3)
        pair, odd = div(c, 2), rem(c, 2)
        forth_k = mid * (2 + odd + 2 * i) + (1 - mid) * (last * (6 + odd) + (1 - last) * pair)
        forth_q = mid * (pair - 2) + (1 - mid) * (2 * (last * (pair - 6) + (1 - last) * odd) + i)
        back_k, back_h = mid * (5 - r) + (1 - mid) * (7 - 6 * last - odd), mid * (q - 1) + (1 - mid) * div(r, 2)
        return back * back_k + (1 - back) * forth_k, back * (2 * back_h + i) + (1 - back) * forth_q

    class Fetch:
        def __init__(self, g):
            self.g, self.slot = g, rem(g, SLOTS)

        def start(self, pieces=(0, 1)):
            for i in pieces:
                k, q = block_quart(self.g, i)
                col = pl.multiple_of(partner(k) * ROWS + q * QUART, QUART)
                pltpu.make_async_copy(adj.at[:, pl.ds(col, QUART)], abuf.at[self.slot, :, pl.ds(i * QUART, QUART)], asem.at[self.slot]).start()

        def wait(self):
            pltpu.make_async_copy(adj.at[:, pl.ds(0, HALF)], abuf.at[self.slot], asem.at[self.slot]).wait()

    fetch = Fetch

    def remote(src, dst, k, send, recv):
        return pltpu.make_async_remote_copy(src_ref=src, dst_ref=dst, send_sem=ssem.at[send], recv_sem=rsem.at[recv],
                                            device_id=(peers[k],), device_id_type=MESH)

    xcopies = [pltpu.make_async_copy(feat.at[:, pl.ds(q * QUART, QUART)], xbuf.at[:, pl.ds(q * QUART, QUART)], xsem.at[5 + q]) for q in range(4)]
    whcopy = pltpu.make_async_copy(wh_in, wh, xsem.at[1])
    whcopy.start()
    for copy in xcopies:
        copy.start()
    small = [pltpu.make_async_copy(src, dst, xsem.at[2 + i]) for i, (src, dst) in
             enumerate(((wo_in, wo), (labels_in, labels), (mask_in, mask)))]
    for copy in small:
        copy.start()
    fetch(0).start()
    barrier = pltpu.get_barrier_semaphore()
    for k in range(1, DEVICES):
        pl.semaphore_signal(barrier, inc=1, device_id=(peers[k],), device_id_type=MESH)
    whcopy.wait()
    wh_t = wh[...].T.astype(BF16)

    def gather_copies(y, send, recv):
        def half(k, h):
            return y.at[k, :, pl.ds(h * HALF, HALF)]

        def quart(k, q):
            return y.at[k, :, pl.ds(q * QUART, QUART)]

        copies = {'own': remote(y.at[0], y.at[1], 1, send, recv)}
        for q in range(4):
            copies['x', q] = remote(quart(0, q), quart(2, q), 2, send, recv + 1 + q)
            copies['y', q] = remote(quart(0, q), quart(4, q), 4, send, recv + 1 + q)
            copies['x core', q] = remote(quart(2, q), quart(3, q), 1, send, recv + 5 + q)
            copies['y core', q] = remote(quart(4, q), quart(5, q), 1, send, recv + 5 + q)
            copies['both', q] = remote(half(0, 0), half(0, 0), 2, send, recv + 1 + q)
            copies['both core', q] = remote(half(0, 0), half(0, 0), 1, send, recv + 5 + q)
            if q % 2 == 0:
                copies['across', q] = remote(quart(2, q), quart(6, q), 4, send, recv + 9 + q // 2)
            else:
                copies['across', q] = remote(quart(4, q), quart(6, q), 2, send, recv + 9 + q // 2)
        for h in range(2):
            copies['across both', h] = remote(half(0, 0), half(0, 0), 2, send, recv + 9 + h)
            copies['across core', h] = remote(half(6, h), half(7, h), 1, send, recv + 11 + h)
        copies['sent'] = remote(y.at[pl.ds(0, 7)], y.at[pl.ds(0, 7)], 1, send, recv)
        return copies

    def gather_start(copies, quarters=range(4)):
        for q in quarters:
            copies['x', q].start()
            copies['y', q].start()
            if q == 3:
                copies['own'].start()

    def gather_need(copies, c):
        if c == 2:
            copies['own'].wait_recv()
        if 4 <= c < 12:
            q = (c - 4) // 2
            if c % 2 == 0:
                copies['both', q].wait_recv()
                copies['across', q].start()
                copies['x core', q].start()
                copies['y core', q].start()
            else:
                copies['both core', q].wait_recv()
        if c >= 12:
            h = (c - 12) // 2
            if c % 2 == 0:
                copies['across both', h].wait_recv()
                copies['across core', h].start()
            else:
                copies['across core', h].wait_recv()

    def mask_value(k):
        return block_mask[me, partner(k)].astype(F32)

    def multiply(y, chunks):
        width = y.shape[1]
        for j, (g, quarters) in enumerate(chunks):
            for part, (k, q) in enumerate(quarters):
                cols = pl.ds(pl.multiple_of(q * QUART, QUART), QUART)
                ymask[:width, (2 * j + part) * QUART:(2 * j + part + 1) * QUART] = (y[k, :, cols].astype(F32) * mask_value(k)).astype(BF16)
        for g, _ in chunks:
            fetch(g).wait()
        for g, _ in chunks:
            fetch(g + SLOTS - 2).start()
        total = None
        for j, (g, _) in enumerate(chunks):
            term = lax.dot_general(abuf[rem(g, SLOTS)], ymask[:width, j * HALF:(j + 1) * HALF], NT, preferred_element_type=F32)
            total = term if total is None else total + term
        acc[:, :width] += total

    copies1 = gather_copies(yall, 0, 0)
    for q in range(4):
        at = pl.ds(q * QUART, QUART)
        xcopies[q].wait()
        yall[0, :, at] = jnp.dot(wh_t, xbuf[:, at], preferred_element_type=F32).astype(BF16)
        if q == 0:
            fetch(1).start()
            pl.semaphore_wait(barrier, DEVICES - 1)
        gather_start(copies1, (q,))
    for g in range(2, SLOTS - 2):
        fetch(g).start()
    acc[...] = jnp.zeros_like(acc)
    for copy in small:
        copy.wait()
    wpad[...] = jnp.zeros_like(wpad)
    wpad[:CLASSES, :] = wo[...]
    cnt[0] = jnp.broadcast_to(jnp.sum(mask[...].astype(F32), axis=1, keepdims=True), (8, 128))
    def own_chip(c, carry):
        @pl.when(c == 2)
        def _():
            gather_need(copies1, 2)
        multiply(yall, [(c, [(lax.div(c, 2), 2 * lax.rem(c, 2) + i) for i in range(2)])])
        return carry
    lax.fori_loop(0, 4, own_chip, 0)

    def need_at(j, steps, first):
        for at in range(steps):
            @pl.when(j == at)
            def _(at=at):
                gather_need(copies1, first + at)

    def neighbours(j, carry):
        need_at(j, 8, 4)
        multiply(yall, [(4 + j, [(2 + lax.rem(j, 2) + 2 * i, lax.div(j, 2)) for i in range(2)])])
        return carry
    lax.fori_loop(0, 8, neighbours, 0)

    def across(j, carry):
        need_at(j, 4, 12)
        multiply(yall, [(12 + j, [(6 + lax.rem(j, 2), 2 * lax.div(j, 2) + i) for i in range(2)])])
        return carry
    lax.fori_loop(0, 4, across, 0)

    hid[...] = jnp.maximum(acc[...], 0.0).astype(BF16)
    y2all[0] = lax.dot_general(wpad[:C_PAD, :].astype(BF16), hid[...], NT, preferred_element_type=F32).astype(BF16)

    copies2 = gather_copies(y2all, 1, 16)
    gather_start(copies2)
    count_copies = [remote(cnt.at[0], cnt.at[k], k, 2, 32) for k in range(1, DEVICES)]
    counts = remote(cnt.at[pl.ds(1, 7)], cnt.at[pl.ds(1, 7)], 1, 2, 32)
    for copy in count_copies:
        copy.start()
    copies1['sent'].wait_send()
    acc[...] = jnp.zeros_like(acc)

    for chunks in ((0, 1), (2, 3), (4,), (5, 6), (7, 8), (9, 10), (11, 12), (13, 14), (15,)):
        for c in chunks:
            gather_need(copies2, c)
        multiply(y2all, [(CHUNKS + c, [block_quart(c, i) for i in range(2)]) for c in chunks])

    for i in range(ROWS // 128):
        at = pl.ds(i * 128, 128)
        pb[0, :C_PAD, at] = acc[at, :].T[:C_PAD]
    counts.wait_recv()
    label_count = cnt[0, 0:1, 0:1]
    for k in range(1, DEVICES):
        label_count = label_count + cnt[k, 0:1, 0:1]
    loss = jnp.zeros((1, 1), F32)
    lhs[C_PAD:, :] = jnp.zeros((HID - C_PAD, ROWS), BF16)
    for q in range(4):
        at = pl.ds(q * QUART, QUART)
        z = pb[0, :C_PAD, at]
        row = lax.broadcasted_iota(jnp.int32, (C_PAD, QUART), 0)
        z = jnp.where(row < CLASSES, z, -jnp.inf)
        top = jnp.max(z, axis=0, keepdims=True)
        log_norm = jnp.log(jnp.sum(jnp.exp(z - top), axis=0, keepdims=True)) + top
        hot = row == labels[:, at]
        picked = jnp.sum(jnp.where(hot, z, 0.0), axis=0, keepdims=True)
        w = mask[:, at].astype(F32)
        loss = loss + jnp.sum(w * (log_norm - picked), axis=1, keepdims=True)
        prob = jnp.exp(z - log_norm)
        lhs[:C_PAD, at] = ((prob - hot.astype(F32)) * (w / label_count)).astype(BF16)

    def scatter_copies(p, r, f, ix, send, recv):
        def half(k, h):
            return p.at[k, :, pl.ds(h * HALF, HALF)]

        def quart(k, q):
            return p.at[k, :, pl.ds(q * QUART, QUART)]

        copies = {'sent': remote(p.at[pl.ds(0, 7)], p.at[pl.ds(0, 7)], 1, send, recv)}
        for h in range(2):
            even, odd = 2 * h, 2 * h + 1
            for k in (7, 5, 3, 1):
                copies['core', k, h] = remote(half(k, h), r.at[k // 2, h], 1, send, recv + k - 1 + h)
            copies['xy', h] = remote(quart(6, even), f.at[0, h], 2, send, recv + 8 + h)
            copies['yx', h] = remote(quart(6, odd), f.at[1, h], 4, send, recv + 10 + h)
            copies['y raw', h] = remote(quart(4, odd), ix.at[1, odd], 4, send, recv + 12 + odd)
            copies['x raw', h] = remote(quart(2, even), ix.at[0, even], 2, send, recv + 12 + even)
            copies['y', h] = remote(quart(4, even), ix.at[1, even], 4, send, recv + 12 + even)
            copies['x', h] = remote(quart(2, odd), ix.at[0, odd], 2, send, recv + 12 + odd)
            copies['both', even] = remote(half(0, 0), half(0, 0), 2, send, recv + 12 + even)
            copies['both', odd] = remote(half(0, 0), half(0, 0), 2, send, recv + 12 + odd)
        return copies

    def scatter_events(copies, p, r, f, c, pass_on):
        sends = {6: ('xy', 'yx'), 4: ('y raw',), 2: ('x raw',), 0: ()}
        order = [(7, 0), (6, 0), (7, 1), (6, 1)] + [(k, h) for h in range(2) for k in (5, 4, 3, 2)] + [(1, 0), (0, 0), (1, 1), (0, 1)]
        for at, (k, h) in enumerate(order):
            @pl.when(c == at)
            def _(at=at, k=k, h=h):
                if k % 2 == 1:
                    copies['core', k, h].start()
                else:
                    cols = pl.ds(h * HALF, HALF)
                    copies['core', k + 1, h].wait_recv()
                    p[k, :, cols] = p[k, :, cols] + r[k // 2, h]
                    for name in sends[k]:
                        copies[name, h].start()
                for way, h2 in pass_on.get(at, ()):
                    if way == 'y':
                        even = pl.ds(2 * h2 * QUART, QUART)
                        copies['xy', h2].wait_recv()
                        p[4, :, even] = p[4, :, even] + f[0, h2]
                    else:
                        odd = pl.ds((2 * h2 + 1) * QUART, QUART)
                        copies['yx', h2].wait_recv()
                        p[2, :, odd] = p[2, :, odd] + f[1, h2]
                    copies[way, h2].start()

    def scatter_result(copies, p, ix, q):
        copies['both', q].wait_recv()
        return (p[0, :, pl.ds(q * QUART, QUART)] + ix[0, q] + ix[1, q]).astype(BF16)

    pa = pb.at[:, pl.ds(0, C_PAD), :]
    copies3 = scatter_copies(pa, ra, fa, ia, 3, 0)

    def pass3(c, carry):
        g = c + 2 * CHUNKS
        k, q = block_quart(g, 0)
        cols = pl.ds(pl.multiple_of(q * QUART, HALF), HALF)
        fetch(g).wait()
        fetch(g + SLOTS - 2).start()
        part = jnp.dot(lhs[...], abuf[rem(g, SLOTS)], preferred_element_type=F32)
        pa[k, :, cols] = part[:C_PAD] * mask_value(k)
        scatter_events(copies3, pa, ra, fa, c, {6: (('y', 0),), 7: (('x', 0),), 9: (('y', 1),), 11: (('x', 1),)})
        return carry
    lax.fori_loop(0, CHUNKS, pass3, 0)
    ident = (lax.broadcasted_iota(jnp.int32, (HID, HID), 0) == lax.broadcasted_iota(jnp.int32, (HID, HID), 1)).astype(BF16)
    hidt[...] = lax.dot_general(ident, hid[...], NT, preferred_element_type=F32).astype(BF16)
    wo_bf = wpad[...].T[:, :C_PAD].astype(BF16)
    copies2['sent'].wait_send()
    d2t = y2all.at[0]
    for q in range(4):
        at = pl.ds(q * QUART, QUART)
        d2t[:, at] = scatter_result(copies3, pa, ia, q)
        back = jnp.dot(wo_bf, d2t[:, at], preferred_element_type=F32)
        lhs[:, at] = jnp.where(hidt[:, at].astype(F32) > 0.0, back, 0.0).astype(BF16)
    copies3['sent'].wait_send()

    copies4 = scatter_copies(pb, rb, fb, ib, 4, 16)

    def pass4(c, carry):
        g = c + 3 * CHUNKS
        k, q = block_quart(g, 0)
        cols = pl.ds(pl.multiple_of(q * QUART, HALF), HALF)
        fetch(g).wait()

        @pl.when(g + SLOTS - 2 < 4 * CHUNKS)
        def _():
            fetch(g + SLOTS - 2).start()
        part = jnp.dot(lhs[...], abuf[rem(g, SLOTS)], preferred_element_type=F32)
        pb[k, :, cols] = part * mask_value(k)
        scatter_events(copies4, pb, rb, fb, c, {9: (('y', 0),), 10: (('x', 0),), 13: (('y', 1), ('x', 1))})
        return carry
    lax.fori_loop(0, CHUNKS, pass4, 0)

    gpart[F_IN // 8 * 8:GWO_ROW, :] = jnp.zeros((8, HID), F32)
    gpart[GWO_ROW:LOSS_ROW, :] = jnp.dot(d2t[...], hid[...], preferred_element_type=F32)
    gpart[LOSS_ROW:SUM_ROWS, :] = jnp.broadcast_to(loss / label_count, (SUM_ROWS - LOSS_ROW, HID))
    counts.wait_send()
    for h in range(2):
        d1t = jnp.concatenate([scatter_result(copies4, pb, ib, 2 * h + q) for q in range(2)], axis=1)
        term = lax.dot_general(xbuf[:, h * HALF:(h + 1) * HALF], d1t, NT, preferred_element_type=F32)
        if h == 0:
            gpart[:F_IN, :] = term
        else:
            gpart[:F_IN, :] += term

    half_rows, quart_rows = SUM_ROWS // 2, SUM_ROWS // 4
    mine = pl.ds(pl.multiple_of(bits[0] * half_rows, 8), half_rows)
    other = pl.ds(pl.multiple_of((1 - bits[0]) * half_rows, 8), half_rows)
    swap = remote(gpart.at[other, :], gpair, 1, 0, 0)
    swap.start()
    swap.wait()
    gpart[mine, :] = gpart[mine, :] + gpair[...]
    first = [{}, {}]
    pieces = [(q, begin, size) for begin, size in ((0, 88), (88, quart_rows - 88)) for q in range(2)]
    rows = []
    for n, (q, begin, size) in enumerate(pieces):
        at = pl.ds(pl.multiple_of(bits[0] * half_rows + q * quart_rows + begin, 8), size)
        rows.append(at)
        for step in range(2):
            way = (2, 4)[(q + step) % 2]
            first[step][n] = remote(gpart.at[at, :], gacross.at[step, q, pl.ds(begin, size), :], way, 5 + 4 * step + n, 1 + 4 * step + n)
        first[0][n].start()
    for step in range(2):
        for n, (q, begin, size) in enumerate(pieces):
            first[step][n].wait()
            gpart[rows[n], :] = gpart[rows[n], :] + gacross[step, q, begin:begin + size, :]
            if step == 0:
                first[1][n].start()
    final = remote(gpart.at[mine, :], sums_out.at[mine, :], 1, 1, 9)
    final.start()
    sums_out[mine, :] = gpart[mine, :]
    copies4['sent'].wait_send()
    final.wait()


def cut_kernel(sums, loss_out, gwh_out, gwo_out):
    gwh_out[...] = sums[:F_IN, :]
    gwo_out[...] = sums[GWO_ROW:GWO_ROW + CLASSES, :]
    loss_out[...] = sums[LOSS_ROW:LOSS_ROW + 1, 0:1]


def device_step(adj, feat, w_hidden, w_output, labels, train_mask, block_mask):
    vmem = pl.BlockSpec(memory_space=pltpu.VMEM)
    hbm = pl.BlockSpec(memory_space=pl.ANY)
    v = pltpu.VMEM
    sends, arrivals = 13, 33
    sums = pl.pallas_call(
        step_kernel,
        out_shape=pltpu.VMEM((SUM_ROWS, HID), F32),
        in_specs=[hbm] * 6 + [pl.BlockSpec(memory_space=pltpu.SMEM)],
        out_specs=vmem,
        scratch_shapes=[
            v((SLOTS, ROWS, HALF), BF16), v((F_IN, ROWS), BF16), v((F_IN, HID), F32), v((CLASSES, HID), F32), v((1, ROWS), jnp.int32), v((1, ROWS), jnp.int32), v((ROWS, HID), F32),
            v((DEVICES, HID, ROWS), BF16), v((DEVICES, C_PAD, ROWS), BF16), v((HID, ROWS), BF16), v((ROWS, HID), BF16),
            v((HID, ROWS), BF16), v((128, 128), F32), v((HID, ROWS), BF16),
            v((DEVICES, 8, 128), F32),
            v((4, 2, C_PAD, HALF), F32), v((2, 2, C_PAD, QUART), F32), v((2, 4, C_PAD, QUART), F32),
            v((DEVICES, HID, ROWS), F32), v((4, 2, HID, HALF), F32), v((2, 2, HID, QUART), F32), v((2, 4, HID, QUART), F32),
            v((SUM_ROWS, HID), F32), v((SUM_ROWS // 2, HID), F32), v((2, 2, SUM_ROWS // 4, HID), F32),
            pltpu.SemaphoreType.DMA((SLOTS,)), pltpu.SemaphoreType.DMA((9,)),
            pltpu.SemaphoreType.DMA((sends,)), pltpu.SemaphoreType.DMA((arrivals,)),
        ],
        compiler_params=pltpu.CompilerParams(collective_id=0, has_side_effects=True, vmem_limit_bytes=62 * 2**20),
        name='gcn_step',
    )(adj, feat.T, w_hidden, w_output.T, labels.reshape(1, ROWS), train_mask.reshape(1, ROWS), block_mask)
    loss, gwh, gwo = pl.pallas_call(
        cut_kernel,
        out_shape=(jax.ShapeDtypeStruct((1, 1), F32), jax.ShapeDtypeStruct((F_IN, HID), F32), jax.ShapeDtypeStruct((CLASSES, HID), F32)),
        in_specs=[vmem],
        out_specs=(vmem, vmem, vmem),
        compiler_params=pltpu.CompilerParams(vmem_limit_bytes=4 * 2**20),
        name='cut',
    )(sums)
    return loss[0, 0], gwh, gwo.T


def solution(mesh):
    row_spec = P(AXIS_NAME, None)
    vec_spec = P(AXIS_NAME)
    return jax.shard_map(device_step, mesh=mesh, in_specs=(row_spec, row_spec, P(), P(), vec_spec, vec_spec, P()), out_specs=(P(), P(), P()), check_vma=False)
```

```python
import jax
import jax.numpy as jnp
from jax import lax
from jax.experimental import pallas as pl
from jax.experimental.pallas import tpu as pltpu
from jax.sharding import PartitionSpec as P

AXIS_NAME = 'nodes'
MESH = pl.DeviceIdType.MESH
F32, BF16 = jnp.float32, jnp.bfloat16
DEVICES = 8
ROWS = 2048
NODES = DEVICES * ROWS
F_IN = 602
HID = 128
CLASSES = 41
C_PAD = 48
HALF = ROWS // 2
QUART = ROWS // 4
SLOTS = 7
CHUNKS = NODES // HALF
SUM_ROWS = 672
GWO_ROW = 608
LOSS_ROW = GWO_ROW + C_PAD
NT = (((1,), (1,)), ((), ()))
BACK_ORDER = ((7, 0), (6, 0), (7, 1), (3, 0), (6, 1), (5, 0), (2, 0), (4, 0), (3, 1), (5, 1), (2, 1), (4, 1), (1, 0), (1, 1), (0, 0), (0, 1))


def div(a, b):
    return a // b if isinstance(a, int) else lax.div(a, b)


def rem(a, b):
    return a % b if isinstance(a, int) else lax.rem(a, b)


def step_kernel(adj, feat, wh_in, wo_in, labels_in, mask_in, block_mask, sums_out,
                abuf, xbuf, wh, wo, labels, mask, acc, yall, y2all, ymask, hid, hidt, wpad, lhs, cnt,
                ra, fa, ia, pb, rb, fb, ib, gpart, gpair, gacross,
                asem, xsem, ssem, rsem):
    me = lax.axis_index(AXIS_NAME)
    bits = (lax.rem(me, 2), lax.rem(me // 2, 2), me // 4)

    def partner(k):
        return lax.rem(bits[0] + k, 2) + 2 * lax.rem(bits[1] + div(k, 2), 2) + 4 * lax.rem(bits[2] + div(k, 4), 2)

    peers = [partner(k) for k in range(DEVICES)]

    def block_quart(g, i):
        back = div(g, 2 * CHUNKS)
        c = rem(g, CHUNKS)
        q = div(c, 4)
        mid = div(q * (3 - q), 2)
        last = div(q, 3)
        pair, odd = div(c, 2), rem(c, 2)
        forth_k = mid * (2 + odd + 2 * i) + (1 - mid) * (last * (6 + odd) + (1 - last) * pair)
        forth_q = mid * (pair - 2) + (1 - mid) * (2 * (last * (pair - 6) + (1 - last) * odd) + i)
        if isinstance(g, int):
            return (BACK_ORDER[c][0], 2 * BACK_ORDER[c][1] + i) if back else (forth_k, forth_q)
        code = jnp.int32(0)
        for at, (k, h) in enumerate(BACK_ORDER):
            code = jnp.where(c == at, 2 * k + h, code)
        return back * div(code, 2) + (1 - back) * forth_k, back * (2 * rem(code, 2) + i) + (1 - back) * forth_q

    class Fetch:
        def __init__(self, g):
            self.g, self.slot = g, rem(g, SLOTS)

        def start(self, pieces=(0, 1)):
            for i in pieces:
                k, q = block_quart(self.g, i)
                col = pl.multiple_of(partner(k) * ROWS + q * QUART, QUART)
                pltpu.make_async_copy(adj.at[:, pl.ds(col, QUART)], abuf.at[self.slot, :, pl.ds(i * QUART, QUART)], asem.at[self.slot]).start()

        def wait(self):
            pltpu.make_async_copy(adj.at[:, pl.ds(0, HALF)], abuf.at[self.slot], asem.at[self.slot]).wait()

    fetch = Fetch

    def remote(src, dst, k, send, recv):
        return pltpu.make_async_remote_copy(src_ref=src, dst_ref=dst, send_sem=ssem.at[send], recv_sem=rsem.at[recv],
                                            device_id=(peers[k],), device_id_type=MESH)

    xcopies = [pltpu.make_async_copy(feat.at[:, pl.ds(q * QUART, QUART)], xbuf.at[:, pl.ds(q * QUART, QUART)], xsem.at[5 + q]) for q in range(4)]
    whcopy = pltpu.make_async_copy(wh_in, wh, xsem.at[1])
    whcopy.start()
    for copy in xcopies:
        copy.start()
    small = [pltpu.make_async_copy(src, dst, xsem.at[2 + i]) for i, (src, dst) in
             enumerate(((wo_in, wo), (labels_in, labels), (mask_in, mask)))]
    for copy in small:
        copy.start()
    fetch(0).start()
    barrier = pltpu.get_barrier_semaphore()
    for k in range(1, DEVICES):
        pl.semaphore_signal(barrier, inc=1, device_id=(peers[k],), device_id_type=MESH)
    whcopy.wait()
    wh_t = wh[...].T.astype(BF16)

    def gather_copies(y, send, recv):
        def half(k, h):
            return y.at[k, :, pl.ds(h * HALF, HALF)]

        def quart(k, q):
            return y.at[k, :, pl.ds(q * QUART, QUART)]

        copies = {'own': remote(y.at[0], y.at[1], 1, send, recv)}
        for q in range(4):
            copies['x', q] = remote(quart(0, q), quart(2, q), 2, send, recv + 1 + q)
            copies['y', q] = remote(quart(0, q), quart(4, q), 4, send, recv + 1 + q)
            copies['x core', q] = remote(quart(2, q), quart(3, q), 1, send, recv + 5 + q)
            copies['y core', q] = remote(quart(4, q), quart(5, q), 1, send, recv + 5 + q)
            copies['both', q] = remote(half(0, 0), half(0, 0), 2, send, recv + 1 + q)
            copies['both core', q] = remote(half(0, 0), half(0, 0), 1, send, recv + 5 + q)
            if q % 2 == 0:
                copies['across', q] = remote(quart(2, q), quart(6, q), 4, send, recv + 9 + q // 2)
            else:
                copies['across', q] = remote(quart(4, q), quart(6, q), 2, send, recv + 9 + q // 2)
        for h in range(2):
            copies['across both', h] = remote(half(0, 0), half(0, 0), 2, send, recv + 9 + h)
            copies['across core', h] = remote(half(6, h), half(7, h), 1, send, recv + 11 + h)
        copies['sent'] = remote(y.at[pl.ds(0, 7)], y.at[pl.ds(0, 7)], 1, send, recv)
        return copies

    def gather_start(copies, quarters=range(4)):
        for q in quarters:
            copies['x', q].start()
            copies['y', q].start()
            if q == 3:
                copies['own'].start()

    def gather_need(copies, c):
        if c == 2:
            copies['own'].wait_recv()
        if 4 <= c < 12:
            q = (c - 4) // 2
            if c % 2 == 0:
                copies['both', q].wait_recv()
                copies['across', q].start()
                copies['x core', q].start()
                copies['y core', q].start()
            else:
                copies['both core', q].wait_recv()
        if c >= 12:
            h = (c - 12) // 2
            if c % 2 == 0:
                copies['across both', h].wait_recv()
                copies['across core', h].start()
            else:
                copies['across core', h].wait_recv()

    def mask_value(k):
        return block_mask[me, partner(k)].astype(F32)

    def multiply(y, chunks):
        width = y.shape[1]
        for j, (g, quarters) in enumerate(chunks):
            for part, (k, q) in enumerate(quarters):
                cols = pl.ds(pl.multiple_of(q * QUART, QUART), QUART)
                ymask[:width, (2 * j + part) * QUART:(2 * j + part + 1) * QUART] = (y[k, :, cols].astype(F32) * mask_value(k)).astype(BF16)
        for g, _ in chunks:
            fetch(g).wait()
        for g, _ in chunks:
            fetch(g + SLOTS - 2).start()
        total = None
        for j, (g, _) in enumerate(chunks):
            term = lax.dot_general(abuf[rem(g, SLOTS)], ymask[:width, j * HALF:(j + 1) * HALF], NT, preferred_element_type=F32)
            total = term if total is None else total + term
        acc[:, :width] += total

    copies1 = gather_copies(yall, 0, 0)
    for q in range(4):
        at = pl.ds(q * QUART, QUART)
        xcopies[q].wait()
        yall[0, :, at] = jnp.dot(wh_t, xbuf[:, at], preferred_element_type=F32).astype(BF16)
        if q == 0:
            fetch(1).start()
            pl.semaphore_wait(barrier, DEVICES - 1)
        gather_start(copies1, (q,))
    for g in range(2, SLOTS - 2):
        fetch(g).start()
    acc[...] = jnp.zeros_like(acc)
    for copy in small:
        copy.wait()
    wpad[...] = jnp.zeros_like(wpad)
    wpad[:CLASSES, :] = wo[...]
    cnt[0] = jnp.broadcast_to(jnp.sum(mask[...].astype(F32), axis=1, keepdims=True), (8, 128))
    def own_chip(c, carry):
        @pl.when(c == 2)
        def _():
            gather_need(copies1, 2)
        multiply(yall, [(c, [(lax.div(c, 2), 2 * lax.rem(c, 2) + i) for i in range(2)])])
        return carry
    lax.fori_loop(0, 4, own_chip, 0)

    def need_at(j, steps, first):
        for at in range(steps):
            @pl.when(j == at)
            def _(at=at):
                gather_need(copies1, first + at)

    def neighbours(j, carry):
        need_at(j, 8, 4)
        multiply(yall, [(4 + j, [(2 + lax.rem(j, 2) + 2 * i, lax.div(j, 2)) for i in range(2)])])
        return carry
    lax.fori_loop(0, 8, neighbours, 0)

    def across(j, carry):
        need_at(j, 4, 12)
        multiply(yall, [(12 + j, [(6 + lax.rem(j, 2), 2 * lax.div(j, 2) + i) for i in range(2)])])
        return carry
    lax.fori_loop(0, 4, across, 0)

    hid[...] = jnp.maximum(acc[...], 0.0).astype(BF16)
    y2all[0] = lax.dot_general(wpad[:C_PAD, :].astype(BF16), hid[...], NT, preferred_element_type=F32).astype(BF16)

    copies2 = gather_copies(y2all, 1, 16)
    gather_start(copies2)
    count_copies = [remote(cnt.at[0], cnt.at[k], k, 2, 32) for k in range(1, DEVICES)]
    counts = remote(cnt.at[pl.ds(1, 7)], cnt.at[pl.ds(1, 7)], 1, 2, 32)
    for copy in count_copies:
        copy.start()
    copies1['sent'].wait_send()
    acc[...] = jnp.zeros_like(acc)

    for chunks in ((0, 1), (2, 3), (4,), (5, 6), (7, 8), (9, 10), (11, 12), (13, 14), (15,)):
        for c in chunks:
            gather_need(copies2, c)
        multiply(y2all, [(CHUNKS + c, [block_quart(c, i) for i in range(2)]) for c in chunks])

    for i in range(ROWS // 128):
        at = pl.ds(i * 128, 128)
        pb[0, :C_PAD, at] = acc[at, :].T[:C_PAD]
    counts.wait_recv()
    label_count = cnt[0, 0:1, 0:1]
    for k in range(1, DEVICES):
        label_count = label_count + cnt[k, 0:1, 0:1]
    loss = jnp.zeros((1, 1), F32)
    lhs[C_PAD:, :] = jnp.zeros((HID - C_PAD, ROWS), BF16)
    for q in range(4):
        at = pl.ds(q * QUART, QUART)
        z = pb[0, :C_PAD, at]
        row = lax.broadcasted_iota(jnp.int32, (C_PAD, QUART), 0)
        z = jnp.where(row < CLASSES, z, -jnp.inf)
        top = jnp.max(z, axis=0, keepdims=True)
        log_norm = jnp.log(jnp.sum(jnp.exp(z - top), axis=0, keepdims=True)) + top
        hot = row == labels[:, at]
        picked = jnp.sum(jnp.where(hot, z, 0.0), axis=0, keepdims=True)
        w = mask[:, at].astype(F32)
        loss = loss + jnp.sum(w * (log_norm - picked), axis=1, keepdims=True)
        prob = jnp.exp(z - log_norm)
        lhs[:C_PAD, at] = ((prob - hot.astype(F32)) * (w / label_count)).astype(BF16)

    def scatter_copies(p, r, f, ix, send, recv):
        def half(k, h):
            return p.at[k, :, pl.ds(h * HALF, HALF)]

        def quart(k, q):
            return p.at[k, :, pl.ds(q * QUART, QUART)]

        copies = {'sent': remote(p.at[pl.ds(0, 7)], p.at[pl.ds(0, 7)], 1, send, recv)}
        for h in range(2):
            even, odd = 2 * h, 2 * h + 1
            for k in (7, 5, 3, 1):
                copies['core', k, h] = remote(half(k, h), r.at[k // 2, h], 1, send, recv + k - 1 + h)
            copies['xy', h] = remote(quart(6, even), f.at[0, h], 2, send, recv + 8 + h)
            copies['yx', h] = remote(quart(6, odd), f.at[1, h], 4, send, recv + 10 + h)
            copies['y raw', h] = remote(quart(4, odd), ix.at[1, odd], 4, send, recv + 12 + odd)
            copies['x raw', h] = remote(quart(2, even), ix.at[0, even], 2, send, recv + 12 + even)
            copies['y', h] = remote(quart(4, even), ix.at[1, even], 4, send, recv + 12 + even)
            copies['x', h] = remote(quart(2, odd), ix.at[0, odd], 2, send, recv + 12 + odd)
            copies['both', even] = remote(half(0, 0), half(0, 0), 2, send, recv + 12 + even)
            copies['both', odd] = remote(half(0, 0), half(0, 0), 2, send, recv + 12 + odd)
        return copies

    def scatter_events(copies, p, r, f, c, pass_on):
        sends = {6: ('xy', 'yx'), 4: ('y raw',), 2: ('x raw',), 0: ()}
        for at, (k, h) in enumerate(BACK_ORDER):
            @pl.when(c == at)
            def _(at=at, k=k, h=h):
                if k % 2 == 1:
                    copies['core', k, h].start()
                else:
                    cols = pl.ds(h * HALF, HALF)
                    copies['core', k + 1, h].wait_recv()
                    p[k, :, cols] = p[k, :, cols] + r[k // 2, h]
                    for name in sends[k]:
                        copies[name, h].start()
                for way, h2 in pass_on.get(at, ()):
                    if way == 'y':
                        even = pl.ds(2 * h2 * QUART, QUART)
                        copies['xy', h2].wait_recv()
                        p[4, :, even] = p[4, :, even] + f[0, h2]
                    else:
                        odd = pl.ds((2 * h2 + 1) * QUART, QUART)
                        copies['yx', h2].wait_recv()
                        p[2, :, odd] = p[2, :, odd] + f[1, h2]
                    copies[way, h2].start()

    def scatter_result(copies, p, ix, q):
        copies['both', q].wait_recv()
        return (p[0, :, pl.ds(q * QUART, QUART)] + ix[0, q] + ix[1, q]).astype(BF16)

    pa = pb.at[:, pl.ds(0, C_PAD), :]
    copies3 = scatter_copies(pa, ra, fa, ia, 3, 0)

    def pass3(c, carry):
        g = c + 2 * CHUNKS
        k, q = block_quart(g, 0)
        cols = pl.ds(pl.multiple_of(q * QUART, HALF), HALF)
        fetch(g).wait()
        fetch(g + SLOTS - 2).start()
        part = jnp.dot(lhs[...], abuf[rem(g, SLOTS)], preferred_element_type=F32)
        pa[k, :, cols] = part[:C_PAD] * mask_value(k)
        scatter_events(copies3, pa, ra, fa, c, {7: (('x', 0), ('y', 0)), 10: (('x', 1),), 11: (('y', 1),)})
        return carry
    lax.fori_loop(0, CHUNKS, pass3, 0)
    ident = (lax.broadcasted_iota(jnp.int32, (HID, HID), 0) == lax.broadcasted_iota(jnp.int32, (HID, HID), 1)).astype(BF16)
    hidt[...] = lax.dot_general(ident, hid[...], NT, preferred_element_type=F32).astype(BF16)
    wo_bf = wpad[...].T[:, :C_PAD].astype(BF16)
    copies2['sent'].wait_send()
    d2t = y2all.at[0]
    for q in range(4):
        at = pl.ds(q * QUART, QUART)
        d2t[:, at] = scatter_result(copies3, pa, ia, q)
        back = jnp.dot(wo_bf, d2t[:, at], preferred_element_type=F32)
        lhs[:, at] = jnp.where(hidt[:, at].astype(F32) > 0.0, back, 0.0).astype(BF16)
    copies3['sent'].wait_send()

    copies4 = scatter_copies(pb, rb, fb, ib, 4, 16)

    def pass4(c, carry):
        g = c + 3 * CHUNKS
        k, q = block_quart(g, 0)
        cols = pl.ds(pl.multiple_of(q * QUART, HALF), HALF)
        fetch(g).wait()

        @pl.when(g + SLOTS - 2 < 4 * CHUNKS)
        def _():
            fetch(g + SLOTS - 2).start()
        part = jnp.dot(lhs[...], abuf[rem(g, SLOTS)], preferred_element_type=F32)
        pb[k, :, cols] = part * mask_value(k)
        scatter_events(copies4, pb, rb, fb, c, {9: (('y', 0), ('x', 0)), 14: (('y', 1), ('x', 1))})
        return carry
    lax.fori_loop(0, CHUNKS, pass4, 0)

    gpart[F_IN // 8 * 8:GWO_ROW, :] = jnp.zeros((8, HID), F32)
    gpart[GWO_ROW:LOSS_ROW, :] = jnp.dot(d2t[...], hid[...], preferred_element_type=F32)
    gpart[LOSS_ROW:SUM_ROWS, :] = jnp.broadcast_to(loss / label_count, (SUM_ROWS - LOSS_ROW, HID))
    counts.wait_send()
    for h in range(2):
        d1t = jnp.concatenate([scatter_result(copies4, pb, ib, 2 * h + q) for q in range(2)], axis=1)
        term = lax.dot_general(xbuf[:, h * HALF:(h + 1) * HALF], d1t, NT, preferred_element_type=F32)
        if h == 0:
            gpart[:F_IN, :] = term
        else:
            gpart[:F_IN, :] += term

    half_rows, quart_rows = SUM_ROWS // 2, SUM_ROWS // 4
    mine = pl.ds(pl.multiple_of(bits[0] * half_rows, 8), half_rows)
    other = pl.ds(pl.multiple_of((1 - bits[0]) * half_rows, 8), half_rows)
    swap = remote(gpart.at[other, :], gpair, 1, 0, 0)
    swap.start()
    swap.wait()
    gpart[mine, :] = gpart[mine, :] + gpair[...]
    first = [{}, {}]
    pieces = [(q, begin, size) for begin, size in ((0, 88), (88, quart_rows - 88)) for q in range(2)]
    rows = []
    for n, (q, begin, size) in enumerate(pieces):
        at = pl.ds(pl.multiple_of(bits[0] * half_rows + q * quart_rows + begin, 8), size)
        rows.append(at)
        for step in range(2):
            way = (2, 4)[(q + step) % 2]
            first[step][n] = remote(gpart.at[at, :], gacross.at[step, q, pl.ds(begin, size), :], way, 5 + 4 * step + n, 1 + 4 * step + n)
        first[0][n].start()
    for step in range(2):
        for n, (q, begin, size) in enumerate(pieces):
            first[step][n].wait()
            gpart[rows[n], :] = gpart[rows[n], :] + gacross[step, q, begin:begin + size, :]
            if step == 0:
                first[1][n].start()
    final = remote(gpart.at[mine, :], sums_out.at[mine, :], 1, 1, 9)
    final.start()
    sums_out[mine, :] = gpart[mine, :]
    copies4['sent'].wait_send()
    final.wait()


def cut_kernel(sums, loss_out, gwh_out, gwo_out):
    gwh_out[...] = sums[:F_IN, :]
    gwo_out[...] = sums[GWO_ROW:GWO_ROW + CLASSES, :]
    loss_out[...] = sums[LOSS_ROW:LOSS_ROW + 1, 0:1]


def device_step(adj, feat, w_hidden, w_output, labels, train_mask, block_mask):
    vmem = pl.BlockSpec(memory_space=pltpu.VMEM)
    hbm = pl.BlockSpec(memory_space=pl.ANY)
    v = pltpu.VMEM
    sends, arrivals = 13, 33
    sums = pl.pallas_call(
        step_kernel,
        out_shape=pltpu.VMEM((SUM_ROWS, HID), F32),
        in_specs=[hbm] * 6 + [pl.BlockSpec(memory_space=pltpu.SMEM)],
        out_specs=vmem,
        scratch_shapes=[
            v((SLOTS, ROWS, HALF), BF16), v((F_IN, ROWS), BF16), v((F_IN, HID), F32), v((CLASSES, HID), F32), v((1, ROWS), jnp.int32), v((1, ROWS), jnp.int32), v((ROWS, HID), F32),
            v((DEVICES, HID, ROWS), BF16), v((DEVICES, C_PAD, ROWS), BF16), v((HID, ROWS), BF16), v((ROWS, HID), BF16),
            v((HID, ROWS), BF16), v((128, 128), F32), v((HID, ROWS), BF16),
            v((DEVICES, 8, 128), F32),
            v((4, 2, C_PAD, HALF), F32), v((2, 2, C_PAD, QUART), F32), v((2, 4, C_PAD, QUART), F32),
            v((DEVICES, HID, ROWS), F32), v((4, 2, HID, HALF), F32), v((2, 2, HID, QUART), F32), v((2, 4, HID, QUART), F32),
            v((SUM_ROWS, HID), F32), v((SUM_ROWS // 2, HID), F32), v((2, 2, SUM_ROWS // 4, HID), F32),
            pltpu.SemaphoreType.DMA((SLOTS,)), pltpu.SemaphoreType.DMA((9,)),
            pltpu.SemaphoreType.DMA((sends,)), pltpu.SemaphoreType.DMA((arrivals,)),
        ],
        compiler_params=pltpu.CompilerParams(collective_id=0, has_side_effects=True, vmem_limit_bytes=62 * 2**20),
        name='gcn_step',
    )(adj, feat.T, w_hidden, w_output.T, labels.reshape(1, ROWS), train_mask.reshape(1, ROWS), block_mask)
    loss, gwh, gwo = pl.pallas_call(
        cut_kernel,
        out_shape=(jax.ShapeDtypeStruct((1, 1), F32), jax.ShapeDtypeStruct((F_IN, HID), F32), jax.ShapeDtypeStruct((CLASSES, HID), F32)),
        in_specs=[vmem],
        out_specs=(vmem, vmem, vmem),
        compiler_params=pltpu.CompilerParams(vmem_limit_bytes=4 * 2**20),
        name='cut',
    )(sums)
    return loss[0, 0], gwh, gwo.T


def solution(mesh):
    row_spec = P(AXIS_NAME, None)
    vec_spec = P(AXIS_NAME)
    return jax.shard_map(device_step, mesh=mesh, in_specs=(row_spec, row_spec, P(), P(), vec_spec, vec_spec, P()), out_specs=(P(), P(), P()), check_vma=False)
```

```python
import jax
import jax.numpy as jnp
from jax import lax
from jax.experimental import pallas as pl
from jax.experimental.pallas import tpu as pltpu
from jax.sharding import PartitionSpec as P

AXIS_NAME = 'nodes'
MESH = pl.DeviceIdType.MESH
F32, BF16 = jnp.float32, jnp.bfloat16
DEVICES = 8
ROWS = 2048
NODES = DEVICES * ROWS
F_IN = 602
HID = 128
CLASSES = 41
C_PAD = 48
HALF = ROWS // 2
QUART = ROWS // 4
SLOTS = 7
CHUNKS = NODES // HALF
SUM_ROWS = 672
GWO_ROW = 608
LOSS_ROW = GWO_ROW + C_PAD
NT = (((1,), (1,)), ((), ()))
BACK_ORDER = ((7, 0), (6, 0), (7, 1), (3, 0), (6, 1), (5, 0), (2, 0), (4, 0), (3, 1), (5, 1), (2, 1), (4, 1), (1, 0), (1, 1), (0, 0), (0, 1))


def div(a, b):
    return a // b if isinstance(a, int) else lax.div(a, b)


def rem(a, b):
    return a % b if isinstance(a, int) else lax.rem(a, b)


def step_kernel(adj, feat, wh_in, wo_in, labels_in, mask_in, block_mask, sums_out,
                abuf, xbuf, wh, wo, labels, mask, acc, yall, y2all, ymask, hid, hidt, wpad, lhs, cnt,
                ra, fa, ia, pb, rb, fb, ib, gpart, gpair, gacross,
                asem, xsem, ssem, rsem):
    me = lax.axis_index(AXIS_NAME)
    bits = (lax.rem(me, 2), lax.rem(me // 2, 2), me // 4)

    def partner(k):
        return lax.rem(bits[0] + k, 2) + 2 * lax.rem(bits[1] + div(k, 2), 2) + 4 * lax.rem(bits[2] + div(k, 4), 2)

    peers = [partner(k) for k in range(DEVICES)]

    def block_quart(g, i):
        back = div(g, 2 * CHUNKS)
        c = rem(g, CHUNKS)
        q = div(c, 4)
        mid = div(q * (3 - q), 2)
        last = div(q, 3)
        pair, odd = div(c, 2), rem(c, 2)
        forth_k = mid * (2 + odd + 2 * i) + (1 - mid) * (last * (6 + odd) + (1 - last) * pair)
        forth_q = mid * (pair - 2) + (1 - mid) * (2 * (last * (pair - 6) + (1 - last) * odd) + i)
        if isinstance(g, int):
            return (BACK_ORDER[c][0], 2 * BACK_ORDER[c][1] + i) if back else (forth_k, forth_q)
        code = jnp.int32(0)
        for at, (k, h) in enumerate(BACK_ORDER):
            code = jnp.where(c == at, 2 * k + h, code)
        return back * div(code, 2) + (1 - back) * forth_k, back * (2 * rem(code, 2) + i) + (1 - back) * forth_q

    class Fetch:
        def __init__(self, g):
            self.g, self.slot = g, rem(g, SLOTS)

        def start(self, pieces=(0, 1)):
            for i in pieces:
                k, q = block_quart(self.g, i)
                col = pl.multiple_of(partner(k) * ROWS + q * QUART, QUART)
                pltpu.make_async_copy(adj.at[:, pl.ds(col, QUART)], abuf.at[self.slot, :, pl.ds(i * QUART, QUART)], asem.at[self.slot]).start()

        def wait(self):
            pltpu.make_async_copy(adj.at[:, pl.ds(0, HALF)], abuf.at[self.slot], asem.at[self.slot]).wait()

    fetch = Fetch

    def remote(src, dst, k, send, recv):
        return pltpu.make_async_remote_copy(src_ref=src, dst_ref=dst, send_sem=ssem.at[send], recv_sem=rsem.at[recv],
                                            device_id=(peers[k],), device_id_type=MESH)

    xcopies = [pltpu.make_async_copy(feat.at[:, pl.ds(q * QUART, QUART)], xbuf.at[:, pl.ds(q * QUART, QUART)], xsem.at[5 + q]) for q in range(4)]
    whcopy = pltpu.make_async_copy(wh_in, wh, xsem.at[1])
    whcopy.start()
    for copy in xcopies:
        copy.start()
    small = [pltpu.make_async_copy(src, dst, xsem.at[2 + i]) for i, (src, dst) in
             enumerate(((wo_in, wo), (labels_in, labels), (mask_in, mask)))]
    for copy in small:
        copy.start()
    fetch(0).start()
    barrier = pltpu.get_barrier_semaphore()
    for k in range(1, DEVICES):
        pl.semaphore_signal(barrier, inc=1, device_id=(peers[k],), device_id_type=MESH)
    whcopy.wait()
    wh_t = wh[...].T.astype(BF16)

    def gather_copies(y, send, recv):
        def half(k, h):
            return y.at[k, :, pl.ds(h * HALF, HALF)]

        def quart(k, q):
            return y.at[k, :, pl.ds(q * QUART, QUART)]

        copies = {'own': remote(y.at[0], y.at[1], 1, send, recv)}
        for q in range(4):
            copies['x', q] = remote(quart(0, q), quart(2, q), 2, send, recv + 1 + q)
            copies['y', q] = remote(quart(0, q), quart(4, q), 4, send, recv + 1 + q)
            copies['x core', q] = remote(quart(2, q), quart(3, q), 1, send, recv + 5 + q)
            copies['y core', q] = remote(quart(4, q), quart(5, q), 1, send, recv + 5 + q)
            copies['both', q] = remote(half(0, 0), half(0, 0), 2, send, recv + 1 + q)
            copies['both core', q] = remote(half(0, 0), half(0, 0), 1, send, recv + 5 + q)
            if q % 2 == 0:
                copies['across', q] = remote(quart(2, q), quart(6, q), 4, send, recv + 9 + q // 2)
            else:
                copies['across', q] = remote(quart(4, q), quart(6, q), 2, send, recv + 9 + q // 2)
        for h in range(2):
            copies['across both', h] = remote(half(0, 0), half(0, 0), 2, send, recv + 9 + h)
            copies['across core', h] = remote(half(6, h), half(7, h), 1, send, recv + 11 + h)
        copies['sent'] = remote(y.at[pl.ds(0, 7)], y.at[pl.ds(0, 7)], 1, send, recv)
        return copies

    def gather_start(copies, quarters=range(4)):
        for q in quarters:
            copies['x', q].start()
            copies['y', q].start()
            if q == 3:
                copies['own'].start()

    def gather_need(copies, c):
        if c == 2:
            copies['own'].wait_recv()
        if 4 <= c < 12:
            q = (c - 4) // 2
            if c % 2 == 0:
                copies['both', q].wait_recv()
                copies['across', q].start()
                copies['x core', q].start()
                copies['y core', q].start()
            else:
                copies['both core', q].wait_recv()
        if c >= 12:
            h = (c - 12) // 2
            if c % 2 == 0:
                copies['across both', h].wait_recv()
                copies['across core', h].start()
            else:
                copies['across core', h].wait_recv()

    def mask_value(k):
        return block_mask[me, partner(k)].astype(F32)

    def multiply(y, chunks):
        width = y.shape[1]
        for j, (g, quarters) in enumerate(chunks):
            for part, (k, q) in enumerate(quarters):
                cols = pl.ds(pl.multiple_of(q * QUART, QUART), QUART)
                ymask[:width, (2 * j + part) * QUART:(2 * j + part + 1) * QUART] = (y[k, :, cols].astype(F32) * mask_value(k)).astype(BF16)
        for g, _ in chunks:
            fetch(g).wait()
        for g, _ in chunks:
            fetch(g + SLOTS - 2).start()
        total = None
        for j, (g, _) in enumerate(chunks):
            term = lax.dot_general(abuf[rem(g, SLOTS)], ymask[:width, j * HALF:(j + 1) * HALF], NT, preferred_element_type=F32)
            total = term if total is None else total + term
        acc[:, :width] += total

    copies1 = gather_copies(yall, 0, 0)
    for q in range(4):
        at = pl.ds(q * QUART, QUART)
        xcopies[q].wait()
        yall[0, :, at] = jnp.dot(wh_t, xbuf[:, at], preferred_element_type=F32).astype(BF16)
        if q == 0:
            fetch(1).start()
            pl.semaphore_wait(barrier, DEVICES - 1)
        gather_start(copies1, (q,))
    for g in range(2, SLOTS - 2):
        fetch(g).start()
    acc[...] = jnp.zeros_like(acc)
    for copy in small:
        copy.wait()
    wpad[...] = jnp.zeros_like(wpad)
    wpad[:CLASSES, :] = wo[...]
    cnt[0] = jnp.broadcast_to(jnp.sum(mask[...].astype(F32), axis=1, keepdims=True), (8, 128))
    def own_chip(c, carry):
        @pl.when(c == 2)
        def _():
            gather_need(copies1, 2)
        multiply(yall, [(c, [(lax.div(c, 2), 2 * lax.rem(c, 2) + i) for i in range(2)])])
        return carry
    lax.fori_loop(0, 4, own_chip, 0)

    def need_at(j, steps, first):
        for at in range(steps):
            @pl.when(j == at)
            def _(at=at):
                gather_need(copies1, first + at)

    def neighbours(j, carry):
        need_at(j, 8, 4)
        multiply(yall, [(4 + j, [(2 + lax.rem(j, 2) + 2 * i, lax.div(j, 2)) for i in range(2)])])
        return carry
    lax.fori_loop(0, 8, neighbours, 0)

    def across(j, carry):
        need_at(j, 4, 12)
        multiply(yall, [(12 + j, [(6 + lax.rem(j, 2), 2 * lax.div(j, 2) + i) for i in range(2)])])
        return carry
    lax.fori_loop(0, 4, across, 0)

    hid[...] = jnp.maximum(acc[...], 0.0).astype(BF16)
    y2all[0] = lax.dot_general(wpad[:C_PAD, :].astype(BF16), hid[...], NT, preferred_element_type=F32).astype(BF16)

    copies2 = gather_copies(y2all, 1, 16)
    gather_start(copies2)
    count_copies = [remote(cnt.at[0], cnt.at[k], k, 2, 32) for k in range(1, DEVICES)]
    counts = remote(cnt.at[pl.ds(1, 7)], cnt.at[pl.ds(1, 7)], 1, 2, 32)
    for copy in count_copies:
        copy.start()
    copies1['sent'].wait_send()
    acc[...] = jnp.zeros_like(acc)

    for chunks in ((0, 1), (2, 3), (4,), (5, 6), (7, 8), (9, 10), (11, 12), (13, 14), (15,)):
        for c in chunks:
            gather_need(copies2, c)
        multiply(y2all, [(CHUNKS + c, [block_quart(c, i) for i in range(2)]) for c in chunks])

    for i in range(ROWS // 128):
        at = pl.ds(i * 128, 128)
        pb[0, :C_PAD, at] = acc[at, :].T[:C_PAD]
    counts.wait_recv()
    label_count = cnt[0, 0:1, 0:1]
    for k in range(1, DEVICES):
        label_count = label_count + cnt[k, 0:1, 0:1]
    loss = jnp.zeros((1, 1), F32)
    lhs[C_PAD:, :] = jnp.zeros((HID - C_PAD, ROWS), BF16)
    for q in range(4):
        at = pl.ds(q * QUART, QUART)
        z = pb[0, :C_PAD, at]
        row = lax.broadcasted_iota(jnp.int32, (C_PAD, QUART), 0)
        z = jnp.where(row < CLASSES, z, -jnp.inf)
        top = jnp.max(z, axis=0, keepdims=True)
        log_norm = jnp.log(jnp.sum(jnp.exp(z - top), axis=0, keepdims=True)) + top
        hot = row == labels[:, at]
        picked = jnp.sum(jnp.where(hot, z, 0.0), axis=0, keepdims=True)
        w = mask[:, at].astype(F32)
        loss = loss + jnp.sum(w * (log_norm - picked), axis=1, keepdims=True)
        prob = jnp.exp(z - log_norm)
        lhs[:C_PAD, at] = ((prob - hot.astype(F32)) * (w / label_count)).astype(BF16)

    def scatter_copies(p, r, f, ix, send, recv):
        def half(k, h):
            return p.at[k, :, pl.ds(h * HALF, HALF)]

        def quart(k, q):
            return p.at[k, :, pl.ds(q * QUART, QUART)]

        copies = {'sent': remote(p.at[pl.ds(0, 7)], p.at[pl.ds(0, 7)], 1, send, recv)}
        for h in range(2):
            even, odd = 2 * h, 2 * h + 1
            for k in (7, 5, 3, 1):
                copies['core', k, h] = remote(half(k, h), r.at[k // 2, h], 1, send, recv + k - 1 + h)
            copies['xy', h] = remote(quart(6, even), f.at[0, h], 2, send, recv + 8 + h)
            copies['yx', h] = remote(quart(6, odd), f.at[1, h], 4, send, recv + 10 + h)
            copies['y raw', h] = remote(quart(4, odd), ix.at[1, odd], 4, send, recv + 12 + odd)
            copies['x raw', h] = remote(quart(2, even), ix.at[0, even], 2, send, recv + 12 + even)
            copies['y', h] = remote(quart(4, even), ix.at[1, even], 4, send, recv + 12 + even)
            copies['x', h] = remote(quart(2, odd), ix.at[0, odd], 2, send, recv + 12 + odd)
            copies['both', even] = remote(half(0, 0), half(0, 0), 2, send, recv + 12 + even)
            copies['both', odd] = remote(half(0, 0), half(0, 0), 2, send, recv + 12 + odd)
        return copies

    def scatter_events(copies, p, r, f, c, pass_on):
        sends = {6: ('xy', 'yx'), 4: ('y raw',), 2: ('x raw',), 0: ()}
        for at, (k, h) in enumerate(BACK_ORDER):
            @pl.when(c == at)
            def _(at=at, k=k, h=h):
                if k % 2 == 1:
                    copies['core', k, h].start()
                else:
                    cols = pl.ds(h * HALF, HALF)
                    copies['core', k + 1, h].wait_recv()
                    p[k, :, cols] = p[k, :, cols] + r[k // 2, h]
                    for name in sends[k]:
                        copies[name, h].start()
                for way, h2 in pass_on.get(at, ()):
                    if way == 'y':
                        even = pl.ds(2 * h2 * QUART, QUART)
                        copies['xy', h2].wait_recv()
                        p[4, :, even] = p[4, :, even] + f[0, h2]
                    else:
                        odd = pl.ds((2 * h2 + 1) * QUART, QUART)
                        copies['yx', h2].wait_recv()
                        p[2, :, odd] = p[2, :, odd] + f[1, h2]
                    copies[way, h2].start()

    def scatter_result(copies, p, ix, q):
        copies['both', q].wait_recv()
        return (p[0, :, pl.ds(q * QUART, QUART)] + ix[0, q] + ix[1, q]).astype(BF16)

    pa = pb.at[:, pl.ds(0, C_PAD), :]
    copies3 = scatter_copies(pa, ra, fa, ia, 3, 0)

    def pass3(c, carry):
        g = c + 2 * CHUNKS
        k, q = block_quart(g, 0)
        cols = pl.ds(pl.multiple_of(q * QUART, HALF), HALF)
        fetch(g).wait()
        fetch(g + SLOTS - 2).start()
        part = jnp.dot(lhs[...], abuf[rem(g, SLOTS)], preferred_element_type=F32)
        pa[k, :, cols] = part[:C_PAD] * mask_value(k)
        scatter_events(copies3, pa, ra, fa, c, {7: (('x', 0), ('y', 0)), 10: (('x', 1),), 11: (('y', 1),)})
        return carry
    lax.fori_loop(0, CHUNKS, pass3, 0)
    ident = (lax.broadcasted_iota(jnp.int32, (HID, HID), 0) == lax.broadcasted_iota(jnp.int32, (HID, HID), 1)).astype(BF16)
    hidt[...] = lax.dot_general(ident, hid[...], NT, preferred_element_type=F32).astype(BF16)
    wo_bf = wpad[...].T[:, :C_PAD].astype(BF16)
    copies2['sent'].wait_send()
    d2t = y2all.at[0]
    for q in range(4):
        at = pl.ds(q * QUART, QUART)
        d2t[:, at] = scatter_result(copies3, pa, ia, q)
        back = jnp.dot(wo_bf, d2t[:, at], preferred_element_type=F32)
        lhs[:, at] = jnp.where(hidt[:, at].astype(F32) > 0.0, back, 0.0).astype(BF16)
    copies3['sent'].wait_send()

    copies4 = scatter_copies(pb, rb, fb, ib, 4, 16)

    def pass4(c, carry):
        g = c + 3 * CHUNKS
        k, q = block_quart(g, 0)
        cols = pl.ds(pl.multiple_of(q * QUART, HALF), HALF)
        fetch(g).wait()

        @pl.when(g + SLOTS - 2 < 4 * CHUNKS)
        def _():
            fetch(g + SLOTS - 2).start()
        part = jnp.dot(lhs[...], abuf[rem(g, SLOTS)], preferred_element_type=F32)
        pb[k, :, cols] = part * mask_value(k)
        scatter_events(copies4, pb, rb, fb, c, {9: (('y', 0), ('x', 0)), 14: (('y', 1), ('x', 1))})
        return carry
    lax.fori_loop(0, CHUNKS, pass4, 0)

    gpart[F_IN // 8 * 8:GWO_ROW, :] = jnp.zeros((8, HID), F32)
    gpart[GWO_ROW:LOSS_ROW, :] = jnp.dot(d2t[...], hid[...], preferred_element_type=F32)
    gpart[LOSS_ROW:SUM_ROWS, :] = jnp.broadcast_to(loss / label_count, (SUM_ROWS - LOSS_ROW, HID))
    counts.wait_send()
    for h in range(2):
        d1t = jnp.concatenate([scatter_result(copies4, pb, ib, 2 * h + q) for q in range(2)], axis=1)
        term = lax.dot_general(xbuf[:, h * HALF:(h + 1) * HALF], d1t, NT, preferred_element_type=F32)
        if h == 0:
            gpart[:F_IN, :] = term
        else:
            gpart[:F_IN, :] += term

    half_rows, quart_rows = SUM_ROWS // 2, SUM_ROWS // 4
    mine = pl.ds(pl.multiple_of(bits[0] * half_rows, 8), half_rows)
    other = pl.ds(pl.multiple_of((1 - bits[0]) * half_rows, 8), half_rows)
    swap = remote(gpart.at[other, :], gpair, 1, 0, 0)
    swap.start()
    swap.wait()
    gpart[mine, :] = gpart[mine, :] + gpair[...]
    first = [{}, {}]
    pieces = [(q, begin, size) for begin, size in ((0, 56), (56, 56), (112, 56)) for q in range(2)]
    rows = []
    for n, (q, begin, size) in enumerate(pieces):
        at = pl.ds(pl.multiple_of(bits[0] * half_rows + q * quart_rows + begin, 8), size)
        rows.append(at)
        for step in range(2):
            way = (2, 4)[(q + step) % 2]
            first[step][n] = remote(gpart.at[at, :], gacross.at[step, q, pl.ds(begin, size), :], way, 5 + 6 * step + n, 1 + 6 * step + n)
        first[0][n].start()
    for step in range(2):
        for n, (q, begin, size) in enumerate(pieces):
            first[step][n].wait()
            gpart[rows[n], :] = gpart[rows[n], :] + gacross[step, q, begin:begin + size, :]
            if step == 0:
                first[1][n].start()
    final = remote(gpart.at[mine, :], sums_out.at[mine, :], 1, 1, 13)
    final.start()
    sums_out[mine, :] = gpart[mine, :]
    copies4['sent'].wait_send()
    final.wait()


def cut_kernel(sums, loss_out, gwh_out, gwo_out):
    gwh_out[...] = sums[:F_IN, :]
    gwo_out[...] = sums[GWO_ROW:GWO_ROW + CLASSES, :]
    loss_out[...] = sums[LOSS_ROW:LOSS_ROW + 1, 0:1]


def device_step(adj, feat, w_hidden, w_output, labels, train_mask, block_mask):
    vmem = pl.BlockSpec(memory_space=pltpu.VMEM)
    hbm = pl.BlockSpec(memory_space=pl.ANY)
    v = pltpu.VMEM
    sends, arrivals = 17, 33
    sums = pl.pallas_call(
        step_kernel,
        out_shape=pltpu.VMEM((SUM_ROWS, HID), F32),
        in_specs=[hbm] * 6 + [pl.BlockSpec(memory_space=pltpu.SMEM)],
        out_specs=vmem,
        scratch_shapes=[
            v((SLOTS, ROWS, HALF), BF16), v((F_IN, ROWS), BF16), v((F_IN, HID), F32), v((CLASSES, HID), F32), v((1, ROWS), jnp.int32), v((1, ROWS), jnp.int32), v((ROWS, HID), F32),
            v((DEVICES, HID, ROWS), BF16), v((DEVICES, C_PAD, ROWS), BF16), v((HID, ROWS), BF16), v((ROWS, HID), BF16),
            v((HID, ROWS), BF16), v((128, 128), F32), v((HID, ROWS), BF16),
            v((DEVICES, 8, 128), F32),
            v((4, 2, C_PAD, HALF), F32), v((2, 2, C_PAD, QUART), F32), v((2, 4, C_PAD, QUART), F32),
            v((DEVICES, HID, ROWS), F32), v((4, 2, HID, HALF), F32), v((2, 2, HID, QUART), F32), v((2, 4, HID, QUART), F32),
            v((SUM_ROWS, HID), F32), v((SUM_ROWS // 2, HID), F32), v((2, 2, SUM_ROWS // 4, HID), F32),
            pltpu.SemaphoreType.DMA((SLOTS,)), pltpu.SemaphoreType.DMA((9,)),
            pltpu.SemaphoreType.DMA((sends,)), pltpu.SemaphoreType.DMA((arrivals,)),
        ],
        compiler_params=pltpu.CompilerParams(collective_id=0, has_side_effects=True, vmem_limit_bytes=62 * 2**20),
        name='gcn_step',
    )(adj, feat.T, w_hidden, w_output.T, labels.reshape(1, ROWS), train_mask.reshape(1, ROWS), block_mask)
    loss, gwh, gwo = pl.pallas_call(
        cut_kernel,
        out_shape=(jax.ShapeDtypeStruct((1, 1), F32), jax.ShapeDtypeStruct((F_IN, HID), F32), jax.ShapeDtypeStruct((CLASSES, HID), F32)),
        in_specs=[vmem],
        out_specs=(vmem, vmem, vmem),
        compiler_params=pltpu.CompilerParams(vmem_limit_bytes=4 * 2**20),
        name='cut',
    )(sums)
    return loss[0, 0], gwh, gwo.T


def solution(mesh):
    row_spec = P(AXIS_NAME, None)
    vec_spec = P(AXIS_NAME)
    return jax.shard_map(device_step, mesh=mesh, in_specs=(row_spec, row_spec, P(), P(), vec_spec, vec_spec, P()), out_specs=(P(), P(), P()), check_vma=False)
```
